512 devices in a mesh: gz: 8 (over z_lo, core), pa: 64 (over y, z_hi, x).
Axes of the slice: x: 4, y: 8, z: 8 (z_hi: 2, z_lo: 4; z = z_hi * 4 + z_lo), core: 2. Of those that a mesh axis runs over, the one named last changes fastest.
Arguments:
- velocity: float32 [3, 8, 2, 512, 1024], P(None, 'gz', None, 'pa'), may hold values from -3 to 3
- mode_mask: int32 [512, 1024], P('pa'), may hold values from 0 to 1, as said below
Outputs:
- velocity_next: float32 [3, 8, 2, 512, 1024], P(None, 'gz', None, 'pa')
- divergence: float32 [8, 2, 512, 1024], P('gz', None, 'pa')
The draws below stay inside these ranges and needn't reach their ends.
Inputs may be any that keep to these rules, and one draw needn't show every extreme that they name: mode_mask is 1 exactly where |s(m)| <= A and n <= B, for one A from 256 to 340 and one B from 256 to 340 in each draw, and 0 elsewhere.
All inputs are finite; a program needn't handle non-finite values.
Results may differ from the reference program's by a relative error of at most 0.00005.
Values sent between devices are 32-bit elements; how exact they have to be, the bound alone decides.
A program may use at most 64 MiB of HBM per device.

```python
import math
import jax
import jax.numpy as jnp
from jax import lax

NX = 1024
NY = 1024
NZ = 8
KY = 512


def draw_mode_mask(key, part):
    first_key = jax.random.fold_in(key, 11)
    second_key = jax.random.fold_in(key, 23)
    cut_x = jax.random.randint(first_key, (), NX // 4, NX // 3)
    cut_y = jax.random.randint(second_key, (), NY // 4, NY // 3)
    modes = jnp.arange(NX, dtype=jnp.int32)
    signed = jnp.where(modes < NX // 2, modes, modes - NX)
    spanwise = jnp.arange(NY // 2, dtype=jnp.int32)
    inside = (jnp.abs(signed)[None, :] <= cut_x) & (spanwise[:, None] <= cut_y)
    return inside.astype(jnp.int32)


def shard_levels(stream_key, dims, shards, low, high):
    gain = 1.0
    for position, blocks in shards:
        steps = jax.random.uniform(jax.random.fold_in(jax.random.fold_in(stream_key, 6), position), (blocks,), jnp.float32, low / len(shards), high / len(shards))
        gain = gain * jnp.repeat(jnp.exp(steps), dims[position] // blocks).reshape((-1,) + (1,) * (len(dims) - 1 - position))
    return gain


def gaussian(key, shape, width, limit, shards=(), kind=jnp.bfloat16):
    factor_of = shard_levels(key, shape, shards, -0.22, 0.18) if shards else 1.0
    drawn = jax.random.normal(key, shape, jnp.float32) * width * factor_of
    return jnp.minimum(jnp.maximum(drawn, -limit), limit).astype(kind)


def setup_inputs(seed: int = 0) -> dict:
    keys = jax.random.split(jax.random.key(seed), 3)
    velocity = gaussian(keys[0], (3, NZ, 2, KY, NX), 0.5, 3.0, ((1, 8), (3, 64)), jnp.float32)
    mode_mask = draw_mode_mask(jax.random.fold_in(keys[2], 71), 0)
    return dict(velocity=velocity, mode_mask=mode_mask)


def wall_first(padded):
    return 0.5 * (padded[2:] - padded[:-2])


def times_wave(wave, field):
    return jnp.stack([-wave * field[:, 1], wave * field[:, 0]], 1)


def reference(velocity, mode_mask):
    half = NY // 2
    modes = jnp.arange(NX, dtype=jnp.int32)
    signed = jnp.where(modes < NX // 2, modes, modes - NX)
    kx_wave = (2.0 * math.pi / NX) * signed.astype(jnp.float32)
    ky_wave = ((2.0 * math.pi / NY) * jnp.arange(half, dtype=jnp.int32).astype(jnp.float32))[:, None]
    padded = jnp.pad(velocity, ((0, 0), (1, 1), (0, 0), (0, 0), (0, 0)))
    u_spec, v_spec, w_spec = velocity[0], velocity[1], velocity[2]
    omega_x = times_wave(ky_wave, w_spec) - wall_first(padded[1])
    omega_y = wall_first(padded[0]) - times_wave(kx_wave, w_spec)
    omega_z = times_wave(kx_wave, v_spec) - times_wave(ky_wave, u_spec)
    spectral = jnp.concatenate([velocity, jnp.stack([omega_x, omega_y, omega_z], 0)], 0)

    def plane(spec):
        coeff = spec[:, 0] + 1j * spec[:, 1]
        columns = jnp.fft.ifft(coeff, axis=2, norm="ortho")
        full = jnp.concatenate([columns, jnp.zeros((6, 1, NX), columns.dtype)], axis=1)
        grid = jnp.fft.irfft(full, n=NY, axis=1, norm="ortho")
        u_grid, v_grid, w_grid, ox_grid, oy_grid, oz_grid = grid[0], grid[1], grid[2], grid[3], grid[4], grid[5]
        cross = jnp.stack([v_grid * oz_grid - w_grid * oy_grid,
                           w_grid * ox_grid - u_grid * oz_grid,
                           u_grid * oy_grid - v_grid * ox_grid], 0)
        rows = jnp.fft.rfft(cross, axis=1, norm="ortho")[:, :half]
        result = jnp.fft.fft(rows, axis=2, norm="ortho")
        return jnp.stack([result.real, result.imag], 1)

    nonlinear = lax.map(plane, jnp.moveaxis(spectral, 1, 0))
    nonlinear = jnp.moveaxis(nonlinear, 0, 1)
    mask = mode_mask.astype(jnp.float32)
    viscous = padded[:, 2:] - 2.0 * padded[:, 1:-1] + padded[:, :-2]
    viscous = viscous - (kx_wave * kx_wave + ky_wave * ky_wave) * velocity
    following = velocity + 0.2 * (nonlinear * mask + 0.25 * viscous)
    w_padded = jnp.pad(following[2], ((1, 1), (0, 0), (0, 0), (0, 0)))
    divergence = times_wave(kx_wave, following[0]) + times_wave(ky_wave, following[1]) + wall_first(w_padded)
    return following, divergence
```

```python
import math

import jax
import jax.numpy as jnp
import numpy as np
from jax import lax
from jax.experimental import pallas as pl
from jax.experimental.pallas import tpu as pltpu
from jax.sharding import PartitionSpec as P


TWO_PI = 2.0 * math.pi
TIME_STEP = 0.2
VISCOSITY = 0.25
RANKS = 64
LAST_RANK = 42
F32 = jnp.float32
BF16 = jnp.bfloat16


def halves(table):
    table = np.asarray(table, np.float32)
    high = table.astype(jnp.bfloat16)
    low = (table - high.astype(np.float32)).astype(jnp.bfloat16)
    return np.stack([high, low])


def tables():
    index = np.arange
    p, b, c, s, q, r = index(64), index(128), index(8), index(8), index(64), index(128)
    d = (2 * p[None, :] + index(2)[:, None]).reshape(-1)
    angle = TWO_PI / 128.0 * (d[:, None] * b[None, :] % 128)
    cos, sin = np.cos(angle) / 32.0, np.sin(angle) / 32.0
    x_in = np.block([[cos, -sin], [sin, cos]])
    angle = TWO_PI / 1024.0 * (c[:, None] * b[None, :])
    x_turn = np.stack([np.cos(angle), np.sin(angle)]).astype(np.float32).reshape(2, 8, 1, 128)
    angle = TWO_PI / 128.0 * (r[:, None] * q[None, :] % 128)
    cos, sin = np.cos(angle) / 32.0, np.sin(angle) / 32.0
    y_in = np.block([[cos, -sin], [sin, cos]])
    angle = TWO_PI / 1024.0 * (r[:, None] * np.tile(s, 16)[None, :])
    y_turn = np.stack([np.cos(angle), np.sin(angle)]).astype(np.float32)
    angle = TWO_PI / 8.0 * (s[:, None] * s[None, :] % 8)
    cos8, sin8 = np.cos(angle), np.sin(angle)
    eye = np.eye(8)
    real = np.kron(np.eye(2), np.kron(eye, cos8))
    imag = np.kron(np.eye(2), np.kron(eye, -sin8))
    both = np.concatenate([real, imag], 0)
    y_grid = np.concatenate([both, np.roll(both, 64, axis=1)], 1)
    real = np.kron(eye, cos8) / 32.0
    imag = np.kron(eye, -sin8) / 32.0
    line = np.concatenate([real, imag, imag, -real], 1)
    y_low = np.concatenate([line, np.zeros_like(line)], 0)
    y_diff = np.concatenate([line, -line], 0)
    angle = TWO_PI / 128.0 * (q[:, None] * r[None, :] % 128)
    y_out = np.concatenate([np.cos(angle), np.sin(angle)], 1)
    angle = TWO_PI / 128.0 * (d[:, None] * b[None, :] % 128)
    x_out = np.concatenate([np.cos(angle), np.sin(angle)], 1) / 32.0
    return dict(
        x_in=halves(x_in),
        x_turn=x_turn,
        y_in=halves(y_in),
        y_turn=y_turn,
        y_grid=halves(y_grid),
        y_low=halves(y_low),
        y_diff=halves(y_diff),
        y_out=halves(y_out),
        x_out=halves(x_out),
    )


NAMES = ("x_in", "x_turn", "y_in", "y_turn", "y_grid", "y_low", "y_diff", "y_out", "x_out")


def split(value):
    high = value.astype(BF16)
    return high, (value - high.astype(F32)).astype(BF16)


def dot(left, right, contract=((1,), (0,))):
    def one(i, j):
        return lax.dot_general(left[i], right[j], (contract, ((), ())), preferred_element_type=F32)

    return one(0, 0) + (one(0, 1) + one(1, 0))


def eight(values, sign):
    count = len(values)
    if count == 1:
        return values
    even, odd = eight(values[0::2], sign), eight(values[1::2], sign)
    half = count // 2
    low, high = [], []
    for k in range(half):
        (er, ei), (qr, qi) = even[k], odd[k]
        turn = 8 // count * k
        if turn == 0:
            tr, ti = qr, qi
        elif turn == 2:
            tr, ti = -sign * qi, sign * qr
        else:
            root = math.sqrt(0.5)
            if turn == 1:
                tr, ti = root * (qr - sign * qi), root * (qi + sign * qr)
            else:
                tr, ti = -root * (qr + sign * qi), root * (sign * qr - qi)
        low.append((er + tr, ei + ti))
        high.append((er - tr, ei - ti))
    return low + high


def x_inverse(fields, turn_cos, turn_sin, table):
    real, imag = [], []
    for field in fields:
        for c, (vr, vi) in enumerate(eight(field, 1.0)):
            real.append(vr * turn_cos[c] - vi * turn_sin[c])
            imag.append(vr * turn_sin[c] + vi * turn_cos[c])
    lines = jnp.concatenate([jnp.concatenate(real, 0), jnp.concatenate(imag, 0)], 1)
    return dot(table, split(lines), ((1,), (1,)))


def y_turned(modes, cos, sin, table):
    lines = dot(table, split(modes))
    out = []
    for k in range(modes.shape[1] // 128):
        vr, vi = lines[:128, 128 * k : 128 * k + 128], lines[128:, 128 * k : 128 * k + 128]
        out.append(jnp.concatenate([vr * cos - vi * sin, vr * sin + vi * cos], 1))
    return out


def y_forward(product, cos, sin, table):
    line = dot(split(product), table)
    one, two = line[:, :128], line[:, 128:]
    return jnp.concatenate([one * cos + two * sin, two * cos - one * sin], 0)


def x_forward(block, turn_cos, turn_sin, table):
    line = dot(split(block.T), table)
    values = []
    for c in range(8):
        re, im = line[8 * c : 8 * c + 8], line[64 + 8 * c : 72 + 8 * c]
        vr, vi = re[:, :128] + im[:, 128:], im[:, :128] - re[:, 128:]
        values.append((vr * turn_cos[c] + vi * turn_sin[c], vi * turn_cos[c] - vr * turn_sin[c]))
    return eight(values, -1.0)


def step(index):
    return (1 - 2 * lax.rem(index, 2)) * lax.div(index + 1, 2)


def partner(me, index):
    dz = 1 - lax.rem(index, 2)
    dx = 2 + step(lax.rem(lax.div(index, 2), 4))
    dy = 4 + step(lax.div(index, 8))
    x = lax.rem(lax.rem(me, 4) + dx, 4)
    z = lax.rem(lax.rem(lax.div(me, 4), 2) + dz, 2)
    y = lax.rem(lax.div(me, 8) + dy, 8)
    return (y * 2 + z) * 4 + x


def rows(start, count):
    return pl.ds(pl.multiple_of(start, count if count != 6 else 8), count)


def kernel(vel, mask, x_in, x_turn, y_in, y_turn, y_grid, y_low, y_diff, y_out, x_out, out, div,
           send_a, recv_a, send_b, recv_b, send_c, recv_c, low, high, w_low, w_high, w_send,
           a_sems, b_sems, c_sems, low_send, low_recv, high_send, high_recv, w_sems):
    me, plane = lax.axis_index("pa"), lax.axis_index("gz")
    barrier = pltpu.get_barrier_semaphore()

    def hello(i, _):
        pl.semaphore_signal(barrier, inc=1, device_id={"gz": plane, "pa": partner(me, i)})
        return 0

    lax.fori_loop(0, RANKS - 1, hello, 0)
    has_low, has_high = plane > 0, plane < 7

    @pl.when(has_low)
    def _():
        pl.semaphore_signal(barrier, inc=1, device_id={"gz": plane - 1, "pa": me})

    @pl.when(has_high)
    def _():
        pl.semaphore_signal(barrier, inc=1, device_id={"gz": plane + 1, "pa": me})

    sub = lax.broadcasted_iota(jnp.int32, (8, 128), 0)
    lane = lax.broadcasted_iota(jnp.int32, (8, 128), 1)
    modes = me * 8 + sub
    ky = (TWO_PI / 1024.0) * modes.astype(F32)
    weight = jnp.where(modes == 0, 1.0, 2.0).astype(F32)

    def kx(a):
        return (TWO_PI / 1024.0) * (lane + (128 * a - 1024 * (a // 4))).astype(F32)

    def piece(ref, *lead):
        return [ref[(*lead, slice(None), pl.ds(128 * a, 128))] for a in range(8)]

    turn_cos = [weight * x_turn[0, c] for c in range(8)]
    turn_sin = [weight * x_turn[1, c] for c in range(8)]

    def field(comp):
        return list(zip(piece(vel, comp, 0, 0), piece(vel, comp, 0, 1), strict=True))

    u, v, w = field(0), field(1), field(2)
    omega_z = [
        (ky * u[a][1] - kx(a) * v[a][1], kx(a) * v[a][0] - ky * u[a][0]) for a in range(8)
    ]
    grid = x_inverse([u, v, w, omega_z], turn_cos, turn_sin, x_in)
    for k in range(2):
        for j in range(4):
            send_a[pl.ds(4 * k + j, 64, stride=8), :] = grid[64 * j : 64 * j + 64, 128 * k : 128 * k + 128]

    @pl.when(jnp.logical_and(has_low, has_high))
    def _():
        pl.semaphore_wait(barrier, RANKS + 1)

    @pl.when(jnp.logical_not(jnp.logical_and(has_low, has_high)))
    def _():
        pl.semaphore_wait(barrier, RANKS)

    def to_low(group):
        comps = pl.ds(0, 2) if group == 0 else pl.ds(2, 1)
        return pltpu.make_async_remote_copy(
            vel.at[comps, 0], high.at[comps], low_send.at[group], high_recv.at[group],
            device_id={"gz": plane - 1, "pa": me})

    def to_high(group):
        comps = pl.ds(0, 2) if group == 0 else pl.ds(2, 1)
        return pltpu.make_async_remote_copy(
            vel.at[comps, 0], low.at[comps], high_send.at[group], low_recv.at[group],
            device_id={"gz": plane + 1, "pa": me})

    @pl.when(has_low)
    def _():
        to_low(0).start()

    @pl.when(has_high)
    def _():
        to_high(0).start()

    def send(source, target, sems, count, stride, dest):
        return pltpu.make_async_remote_copy(
            source.at[rows(dest * stride, count)], target.at[rows(me * stride, count)],
            sems.at[0], sems.at[1], device_id={"gz": plane, "pa": dest})

    def start_a(i, _):
        send(send_a, recv_a, a_sems, 8, 8, partner(me, i)).start()
        return 0

    lax.fori_loop(0, RANKS - 1, start_a, 0)

    @pl.when(has_low)
    def _():
        to_low(1).start()
        pltpu.make_async_copy(low.at[pl.ds(0, 2)], low.at[pl.ds(0, 2)], low_recv.at[0]).wait()

    @pl.when(jnp.logical_not(has_low))
    def _():
        low[...] = jnp.zeros_like(low)
        w_low[...] = jnp.zeros_like(w_low)

    @pl.when(has_high)
    def _():
        to_high(1).start()
        pltpu.make_async_copy(high.at[pl.ds(0, 2)], high.at[pl.ds(0, 2)], high_recv.at[0]).wait()

    @pl.when(jnp.logical_not(has_high))
    def _():
        high[...] = jnp.zeros_like(high)
        w_high[...] = jnp.zeros_like(w_high)

    def slope(comp):
        pairs = []
        for a in range(8):
            at = pl.ds(128 * a, 128)
            pairs.append(tuple(0.5 * (high[comp, i, :, at] - low[comp, i, :, at]) for i in range(2)))
        return pairs

    dz_u, dz_v = slope(0), slope(1)
    w = field(2)
    omega_x = [(-(ky * w[a][1]) - dz_v[a][0], ky * w[a][0] - dz_v[a][1]) for a in range(8)]
    omega_y = [(dz_u[a][0] + kx(a) * w[a][1], dz_u[a][1] - kx(a) * w[a][0]) for a in range(8)]
    grid = x_inverse([omega_x, omega_y], turn_cos, turn_sin, x_in)
    for j in range(4):
        send_b[pl.ds(j, 64, stride=4), :] = grid[64 * j : 64 * j + 64]

    def start_b(i, _):
        send(send_b, recv_b, b_sems, 4, 4, partner(me, i)).start()
        return 0

    lax.fori_loop(0, RANKS - 1, start_b, 0)
    recv_a[rows(me * 8, 8), :] = send_a[rows(me * 8, 8), :]
    recv_b[rows(me * 4, 4), :] = send_b[rows(me * 4, 4), :]

    def wait_all(ref, sem, count):
        view = ref.at[pl.ds(0, count)]
        pltpu.make_async_copy(view, view, sem).wait()

    cos, sin = y_turn[0], y_turn[1]
    wait_all(recv_a, a_sems.at[1], 8 * (RANKS - 1))

    def gathered(ref, stride, base, e):
        return jnp.concatenate(
            [ref[pl.ds(base + e, 64, stride=stride), :], ref[pl.ds(base + 2 + e, 64, stride=stride), :]], 0)

    first = y_turned(
        jnp.concatenate([gathered(recv_a, 8, 4 * k, e) for k in range(2) for e in range(2)], 1), cos, sin, y_in)
    first = [dot(split(value), y_grid) for value in first]
    wait_all(recv_b, b_sems.at[1], 4 * (RANKS - 1))
    second = y_turned(jnp.concatenate([gathered(recv_b, 4, 0, e) for e in range(2)], 1), cos, sin, y_in)
    second = [dot(split(value), y_grid) for value in second]

    def last(parts):
        return dot(y_out, split(jnp.concatenate(parts, 1)))

    products = [[], [], []]
    for e in range(2):
        uv, wz, xy = first[e], first[2 + e], second[e]
        uv, vu = uv[:, :128], uv[:, 128:]
        wz, zw = wz[:, :128], wz[:, 128:]
        xy, yx = xy[:, :128], xy[:, 128:]
        products[0].append(vu * zw - wz * yx)
        products[1].append(wz * xy - uv * zw)
        products[2].append(uv * yx)
    for comp in range(3):
        table = y_diff if comp == 2 else y_low
        spectral = last([y_forward(value, cos, sin, table) for value in products[comp]])
        for e in range(2):
            send_c[pl.ds(2 * comp + e, 64, stride=8), :] = spectral[:, 128 * e : 128 * e + 128]

    def start_c(i, _):
        dest = partner(me, i)

        @pl.when(dest <= LAST_RANK)
        def _():
            send(send_c, recv_c, c_sems, 6, 8, dest).start()

        return 0

    lax.fori_loop(0, RANKS - 1, start_c, 0)
    inside = me <= LAST_RANK

    @pl.when(has_low)
    def _():
        pltpu.make_async_copy(low.at[pl.ds(2, 1)], low.at[pl.ds(2, 1)], low_recv.at[1]).wait()

    @pl.when(has_high)
    def _():
        pltpu.make_async_copy(high.at[pl.ds(2, 1)], high.at[pl.ds(2, 1)], high_recv.at[1]).wait()

    for comp in range(3):
        for i in range(2):
            for a in range(8):
                at = pl.ds(128 * a, 128)
                mid = vel[comp, 0, i, :, at]
                viscous = (high[comp, i, :, at] - 2.0 * mid + low[comp, i, :, at]) - (kx(a) * kx(a) + ky * ky) * mid
                out[comp, 0, i, :, at] = mid + (TIME_STEP * VISCOSITY) * viscous

    @pl.when(inside)
    def _():
        recv_c[rows(me * 8, 6), :] = send_c[rows(me * 8, 6), :]
        wait_all(recv_c, c_sems.at[1], 6 * (RANKS - 1))
        plain_cos = [jnp.broadcast_to(x_turn[0, c], (8, 128)) for c in range(8)]
        plain_sin = [jnp.broadcast_to(x_turn[1, c], (8, 128)) for c in range(8)]
        for comp in range(3):
            block = jnp.concatenate([recv_c[pl.ds(2 * comp + e, 64, stride=8), :] for e in range(2)], 0)
            for a, pair in enumerate(x_forward(block, plain_cos, plain_sin, x_out)):
                at = pl.ds(128 * a, 128)
                keep = mask[:, at].astype(F32) * TIME_STEP
                for i in range(2):
                    out[comp, 0, i, :, at] = out[comp, 0, i, :, at] + pair[i] * keep

    w_send[...] = out[2, 0]

    def w_to_low():
        return pltpu.make_async_remote_copy(
            w_send, w_high, w_sems.at[0], w_sems.at[1], device_id={"gz": plane - 1, "pa": me})

    def w_to_high():
        return pltpu.make_async_remote_copy(
            w_send, w_low, w_sems.at[2], w_sems.at[3], device_id={"gz": plane + 1, "pa": me})

    @pl.when(has_low)
    def _():
        w_to_low().start()

    @pl.when(has_high)
    def _():
        w_to_high().start()

    for a in range(8):
        at = pl.ds(128 * a, 128)
        div[0, 0, :, at] = -(kx(a) * out[0, 0, 1, :, at]) - ky * out[1, 0, 1, :, at]
        div[0, 1, :, at] = kx(a) * out[0, 0, 0, :, at] + ky * out[1, 0, 0, :, at]

    @pl.when(has_low)
    def _():
        pltpu.make_async_copy(w_low, w_low, w_sems.at[3]).wait()

    @pl.when(has_high)
    def _():
        pltpu.make_async_copy(w_high, w_high, w_sems.at[1]).wait()

    div[0] = div[0] + 0.5 * (w_high[...] - w_low[...])

    wait_all(send_a, a_sems.at[0], 8 * (RANKS - 1))
    wait_all(send_b, b_sems.at[0], 4 * (RANKS - 1))

    @pl.when(inside)
    def _():
        wait_all(send_c, c_sems.at[0], 6 * LAST_RANK)

    @pl.when(jnp.logical_not(inside))
    def _():
        wait_all(send_c, c_sems.at[0], 6 * (LAST_RANK + 1))

    @pl.when(has_low)
    def _():
        to_low(0).wait_send()
        to_low(1).wait_send()
        w_to_low().wait_send()

    @pl.when(has_high)
    def _():
        to_high(0).wait_send()
        to_high(1).wait_send()
        w_to_high().wait_send()


def on_device(velocity, mode_mask):
    constants = tables()
    whole = pl.BlockSpec(memory_space=pltpu.VMEM)
    dma, vmem = pltpu.SemaphoreType.DMA, pltpu.VMEM
    return pl.pallas_call(
        kernel,
        name="substep",
        out_shape=(
            jax.ShapeDtypeStruct((3, 1, 2, 8, 1024), F32),
            jax.ShapeDtypeStruct((1, 2, 8, 1024), F32),
        ),
        in_specs=[whole] * (2 + len(NAMES)),
        out_specs=(whole, whole),
        scratch_shapes=[
            vmem((512, 128), F32), vmem((512, 128), F32),
            vmem((256, 128), F32), vmem((256, 128), F32),
            vmem((512, 128), F32), vmem((512, 128), F32),
            vmem((3, 2, 8, 1024), F32), vmem((3, 2, 8, 1024), F32),
            vmem((2, 8, 1024), F32), vmem((2, 8, 1024), F32), vmem((2, 8, 1024), F32),
            dma((2,)), dma((2,)), dma((2,)),
            dma((2,)), dma((2,)), dma((2,)), dma((2,)), dma((4,)),
        ],
        compiler_params=pltpu.CompilerParams(collective_id=0, has_side_effects=True),
    )(velocity, mode_mask, *(jnp.asarray(constants[name]) for name in NAMES))


def solution(mesh):
    return jax.shard_map(
        on_device,
        mesh=mesh,
        in_specs=(P(None, "gz", None, "pa", None), P("pa", None)),
        out_specs=(P(None, "gz", None, "pa", None), P("gz", None, "pa", None)),
        check_vma=False,
    )
```

```python
import math

import jax
import jax.numpy as jnp
import numpy as np
from jax import lax
from jax.experimental import pallas as pl
from jax.experimental.pallas import tpu as pltpu
from jax.sharding import PartitionSpec as P


TWO_PI = 2.0 * math.pi
TIME_STEP = 0.2
VISCOSITY = 0.25
RANKS = 64
LAST_RANK = 42
F32 = jnp.float32
BF16 = jnp.bfloat16


def halves(table):
    table = np.asarray(table, np.float32)
    high = table.astype(jnp.bfloat16)
    low = (table - high.astype(np.float32)).astype(jnp.bfloat16)
    return np.stack([high, low])


def tables():
    index = np.arange
    p, b, c, s, q, r = index(64), index(128), index(8), index(8), index(64), index(128)
    d = (2 * p[None, :] + index(2)[:, None]).reshape(-1)
    angle = TWO_PI / 128.0 * (d[:, None] * b[None, :] % 128)
    cos, sin = np.cos(angle) / 32.0, np.sin(angle) / 32.0
    x_in = np.block([[cos, -sin], [sin, cos]])
    angle = TWO_PI / 1024.0 * (c[:, None] * b[None, :])
    x_turn = np.stack([np.cos(angle), np.sin(angle)]).astype(np.float32).reshape(2, 8, 1, 128)
    angle = TWO_PI / 128.0 * (r[:, None] * q[None, :] % 128)
    cos, sin = np.cos(angle) / 32.0, np.sin(angle) / 32.0
    y_in = np.block([[cos, -sin], [sin, cos]])
    angle = TWO_PI / 1024.0 * (r[:, None] * np.tile(s, 16)[None, :])
    y_turn = np.stack([np.cos(angle), np.sin(angle)]).astype(np.float32)
    angle = TWO_PI / 8.0 * (s[:, None] * s[None, :] % 8)
    cos8, sin8 = np.cos(angle), np.sin(angle)
    eye = np.eye(8)
    real = np.kron(np.eye(2), np.kron(eye, cos8))
    imag = np.kron(np.eye(2), np.kron(eye, -sin8))
    both = np.concatenate([real, imag], 0)
    y_grid = np.concatenate([both, np.roll(both, 64, axis=1)], 1)
    real = np.kron(eye, cos8) / 32.0
    imag = np.kron(eye, -sin8) / 32.0
    line = np.concatenate([real, imag, imag, -real], 1)
    y_low = np.concatenate([line, np.zeros_like(line)], 0)
    y_diff = np.concatenate([line, -line], 0)
    angle = TWO_PI / 128.0 * (q[:, None] * r[None, :] % 128)
    y_out = np.concatenate([np.cos(angle), np.sin(angle)], 1)
    angle = TWO_PI / 128.0 * (d[:, None] * b[None, :] % 128)
    x_out = np.concatenate([np.cos(angle), np.sin(angle)], 1) / 32.0
    return dict(
        x_in=halves(x_in),
        x_turn=x_turn,
        y_in=halves(y_in),
        y_turn=y_turn,
        y_grid=halves(y_grid),
        y_low=halves(y_low),
        y_diff=halves(y_diff),
        y_out=halves(y_out),
        x_out=halves(x_out),
    )


NAMES = ("x_in", "x_turn", "y_in", "y_turn", "y_grid", "y_low", "y_diff", "y_out", "x_out")


def split(value):
    high = value.astype(BF16)
    return high, (value - high.astype(F32)).astype(BF16)


def dot(left, right, contract=((1,), (0,))):
    def one(i, j):
        return lax.dot_general(left[i], right[j], (contract, ((), ())), preferred_element_type=F32)

    return one(0, 0) + (one(0, 1) + one(1, 0))


def eight(values, sign):
    count = len(values)
    if count == 1:
        return values
    even, odd = eight(values[0::2], sign), eight(values[1::2], sign)
    half = count // 2
    low, high = [], []
    for k in range(half):
        (er, ei), (qr, qi) = even[k], odd[k]
        turn = 8 // count * k
        if turn == 0:
            tr, ti = qr, qi
        elif turn == 2:
            tr, ti = -sign * qi, sign * qr
        else:
            root = math.sqrt(0.5)
            if turn == 1:
                tr, ti = root * (qr - sign * qi), root * (qi + sign * qr)
            else:
                tr, ti = -root * (qr + sign * qi), root * (sign * qr - qi)
        low.append((er + tr, ei + ti))
        high.append((er - tr, ei - ti))
    return low + high


def x_inverse(fields, turn_cos, turn_sin, table):
    real, imag = [], []
    for field in fields:
        for c, (vr, vi) in enumerate(eight(field, 1.0)):
            real.append(vr * turn_cos[c] - vi * turn_sin[c])
            imag.append(vr * turn_sin[c] + vi * turn_cos[c])
    lines = jnp.concatenate([jnp.concatenate(real, 0), jnp.concatenate(imag, 0)], 1)
    return dot(table, split(lines), ((1,), (1,)))


def y_turned(modes, cos, sin, table):
    lines = dot(table, split(modes))
    out = []
    for k in range(modes.shape[1] // 128):
        vr, vi = lines[:128, 128 * k : 128 * k + 128], lines[128:, 128 * k : 128 * k + 128]
        out.append(jnp.concatenate([vr * cos - vi * sin, vr * sin + vi * cos], 1))
    return out


def y_forward(product, cos, sin, table):
    line = dot(split(product), table)
    one, two = line[:, :128], line[:, 128:]
    return jnp.concatenate([one * cos + two * sin, two * cos - one * sin], 0)


def x_forward(block, turn_cos, turn_sin, table):
    line = dot(split(block.T), table)
    values = []
    for c in range(8):
        re, im = line[8 * c : 8 * c + 8], line[64 + 8 * c : 72 + 8 * c]
        vr, vi = re[:, :128] + im[:, 128:], im[:, :128] - re[:, 128:]
        values.append((vr * turn_cos[c] + vi * turn_sin[c], vi * turn_cos[c] - vr * turn_sin[c]))
    return eight(values, -1.0)


def step(index):
    return (1 - 2 * lax.rem(index, 2)) * lax.div(index + 1, 2)


def partner(me, index):
    dz = 1 - lax.rem(index, 2)
    dx = 2 + step(lax.rem(lax.div(index, 2), 4))
    dy = 4 + step(lax.div(index, 8))
    x = lax.rem(lax.rem(me, 4) + dx, 4)
    z = lax.rem(lax.rem(lax.div(me, 4), 2) + dz, 2)
    y = lax.rem(lax.div(me, 8) + dy, 8)
    return (y * 2 + z) * 4 + x


def rows(start, count):
    return pl.ds(pl.multiple_of(start, count if count != 6 else 8), count)


def kernel(*refs):
    count = 2 + len(NAMES)
    sources, out, div, held = refs[:count], refs[count], refs[count + 1], refs[count + 2 : 2 * count + 2]
    body(sources, held, out, div, *refs[2 * count + 2 :])


def body(sources, held, out, div, load_sems,
           send_a, recv_a, send_b, recv_b, send_c, recv_c, low, high, w_low, w_high, w_send,
           a_sems, b_sems, c_sems, low_send, low_recv, high_send, high_recv, w_sems):
    me, plane = lax.axis_index("pa"), lax.axis_index("gz")
    barrier = pltpu.get_barrier_semaphore()
    vel, mask, x_in, x_turn, y_in, y_turn, y_grid, y_low, y_diff, y_out, x_out = held

    def load(i):
        return pltpu.make_async_copy(sources[i], held[i], load_sems.at[i])

    for i in (0, 2, 3):
        load(i).start()

    def hello(i, _):
        pl.semaphore_signal(barrier, inc=1, device_id={"gz": plane, "pa": partner(me, i)})
        return 0

    lax.fori_loop(0, RANKS - 1, hello, 0)
    has_low, has_high = plane > 0, plane < 7

    @pl.when(has_low)
    def _():
        pl.semaphore_signal(barrier, inc=1, device_id={"gz": plane - 1, "pa": me})

    @pl.when(has_high)
    def _():
        pl.semaphore_signal(barrier, inc=1, device_id={"gz": plane + 1, "pa": me})

    rest = [i for i in range(len(held)) if i not in (0, 2, 3)]
    for i in rest:
        load(i).start()
    sub = lax.broadcasted_iota(jnp.int32, (8, 128), 0)
    lane = lax.broadcasted_iota(jnp.int32, (8, 128), 1)
    modes = me * 8 + sub
    ky = (TWO_PI / 1024.0) * modes.astype(F32)
    weight = jnp.where(modes == 0, 1.0, 2.0).astype(F32)

    def kx(a):
        return (TWO_PI / 1024.0) * (lane + (128 * a - 1024 * (a // 4))).astype(F32)

    def piece(ref, *lead):
        return [ref[(*lead, slice(None), pl.ds(128 * a, 128))] for a in range(8)]

    for i in (0, 2, 3):
        load(i).wait()
    turn_cos = [weight * x_turn[0, c] for c in range(8)]
    turn_sin = [weight * x_turn[1, c] for c in range(8)]

    def field(comp):
        return list(zip(piece(vel, comp, 0, 0), piece(vel, comp, 0, 1), strict=True))

    u, v, w = field(0), field(1), field(2)
    omega_z = [
        (ky * u[a][1] - kx(a) * v[a][1], kx(a) * v[a][0] - ky * u[a][0]) for a in range(8)
    ]
    grid = x_inverse([u, v, w, omega_z], turn_cos, turn_sin, x_in)
    for k in range(2):
        for j in range(4):
            send_a[pl.ds(4 * k + j, 64, stride=8), :] = grid[64 * j : 64 * j + 64, 128 * k : 128 * k + 128]

    @pl.when(jnp.logical_and(has_low, has_high))
    def _():
        pl.semaphore_wait(barrier, RANKS + 1)

    @pl.when(jnp.logical_not(jnp.logical_and(has_low, has_high)))
    def _():
        pl.semaphore_wait(barrier, RANKS)

    def to_low(group):
        comps = pl.ds(0, 2) if group == 0 else pl.ds(2, 1)
        return pltpu.make_async_remote_copy(
            vel.at[comps, 0], high.at[comps], low_send.at[group], high_recv.at[group],
            device_id={"gz": plane - 1, "pa": me})

    def to_high(group):
        comps = pl.ds(0, 2) if group == 0 else pl.ds(2, 1)
        return pltpu.make_async_remote_copy(
            vel.at[comps, 0], low.at[comps], high_send.at[group], low_recv.at[group],
            device_id={"gz": plane + 1, "pa": me})

    @pl.when(has_low)
    def _():
        to_low(0).start()

    @pl.when(has_high)
    def _():
        to_high(0).start()

    def send(source, target, sems, count, stride, dest):
        return pltpu.make_async_remote_copy(
            source.at[rows(dest * stride, count)], target.at[rows(me * stride, count)],
            sems.at[0], sems.at[1], device_id={"gz": plane, "pa": dest})

    def start_a(i, _):
        send(send_a, recv_a, a_sems, 8, 8, partner(me, i)).start()
        return 0

    lax.fori_loop(0, RANKS - 1, start_a, 0)

    @pl.when(has_low)
    def _():
        to_low(1).start()
        pltpu.make_async_copy(low.at[pl.ds(0, 2)], low.at[pl.ds(0, 2)], low_recv.at[0]).wait()

    @pl.when(jnp.logical_not(has_low))
    def _():
        low[...] = jnp.zeros_like(low)
        w_low[...] = jnp.zeros_like(w_low)

    @pl.when(has_high)
    def _():
        to_high(1).start()
        pltpu.make_async_copy(high.at[pl.ds(0, 2)], high.at[pl.ds(0, 2)], high_recv.at[0]).wait()

    @pl.when(jnp.logical_not(has_high))
    def _():
        high[...] = jnp.zeros_like(high)
        w_high[...] = jnp.zeros_like(w_high)

    def slope(comp):
        pairs = []
        for a in range(8):
            at = pl.ds(128 * a, 128)
            pairs.append(tuple(0.5 * (high[comp, i, :, at] - low[comp, i, :, at]) for i in range(2)))
        return pairs

    dz_u, dz_v = slope(0), slope(1)
    w = field(2)
    omega_x = [(-(ky * w[a][1]) - dz_v[a][0], ky * w[a][0] - dz_v[a][1]) for a in range(8)]
    omega_y = [(dz_u[a][0] + kx(a) * w[a][1], dz_u[a][1] - kx(a) * w[a][0]) for a in range(8)]
    grid = x_inverse([omega_x, omega_y], turn_cos, turn_sin, x_in)
    for j in range(4):
        send_b[pl.ds(j, 64, stride=4), :] = grid[64 * j : 64 * j + 64]

    def start_b(i, _):
        send(send_b, recv_b, b_sems, 4, 4, partner(me, i)).start()
        return 0

    lax.fori_loop(0, RANKS - 1, start_b, 0)
    recv_a[rows(me * 8, 8), :] = send_a[rows(me * 8, 8), :]
    recv_b[rows(me * 4, 4), :] = send_b[rows(me * 4, 4), :]

    def wait_all(ref, sem, count):
        view = ref.at[pl.ds(0, count)]
        pltpu.make_async_copy(view, view, sem).wait()

    for i in rest:
        load(i).wait()
    cos, sin = y_turn[0], y_turn[1]
    wait_all(recv_a, a_sems.at[1], 8 * (RANKS - 1))

    def gathered(ref, stride, base, e):
        return jnp.concatenate(
            [ref[pl.ds(base + e, 64, stride=stride), :], ref[pl.ds(base + 2 + e, 64, stride=stride), :]], 0)

    first = y_turned(
        jnp.concatenate([gathered(recv_a, 8, 4 * k, e) for k in range(2) for e in range(2)], 1), cos, sin, y_in)
    first = [dot(split(value), y_grid) for value in first]
    wait_all(recv_b, b_sems.at[1], 4 * (RANKS - 1))
    second = y_turned(jnp.concatenate([gathered(recv_b, 4, 0, e) for e in range(2)], 1), cos, sin, y_in)
    second = [dot(split(value), y_grid) for value in second]

    def last(parts):
        return dot(y_out, split(jnp.concatenate(parts, 1)))

    products = [[], [], []]
    for e in range(2):
        uv, wz, xy = first[e], first[2 + e], second[e]
        uv, vu = uv[:, :128], uv[:, 128:]
        wz, zw = wz[:, :128], wz[:, 128:]
        xy, yx = xy[:, :128], xy[:, 128:]
        products[0].append(vu * zw - wz * yx)
        products[1].append(wz * xy - uv * zw)
        products[2].append(uv * yx)
    for comp in range(3):
        table = y_diff if comp == 2 else y_low
        spectral = last([y_forward(value, cos, sin, table) for value in products[comp]])
        for e in range(2):
            send_c[pl.ds(2 * comp + e, 64, stride=8), :] = spectral[:, 128 * e : 128 * e + 128]

    def start_c(i, _):
        dest = partner(me, i)

        @pl.when(dest <= LAST_RANK)
        def _():
            send(send_c, recv_c, c_sems, 6, 8, dest).start()

        return 0

    lax.fori_loop(0, RANKS - 1, start_c, 0)
    inside = me <= LAST_RANK

    @pl.when(has_low)
    def _():
        pltpu.make_async_copy(low.at[pl.ds(2, 1)], low.at[pl.ds(2, 1)], low_recv.at[1]).wait()

    @pl.when(has_high)
    def _():
        pltpu.make_async_copy(high.at[pl.ds(2, 1)], high.at[pl.ds(2, 1)], high_recv.at[1]).wait()

    for comp in range(3):
        for i in range(2):
            for a in range(8):
                at = pl.ds(128 * a, 128)
                mid = vel[comp, 0, i, :, at]
                viscous = (high[comp, i, :, at] - 2.0 * mid + low[comp, i, :, at]) - (kx(a) * kx(a) + ky * ky) * mid
                out[comp, 0, i, :, at] = mid + (TIME_STEP * VISCOSITY) * viscous

    @pl.when(inside)
    def _():
        recv_c[rows(me * 8, 6), :] = send_c[rows(me * 8, 6), :]
        wait_all(recv_c, c_sems.at[1], 6 * (RANKS - 1))
        plain_cos = [jnp.broadcast_to(x_turn[0, c], (8, 128)) for c in range(8)]
        plain_sin = [jnp.broadcast_to(x_turn[1, c], (8, 128)) for c in range(8)]
        for comp in range(3):
            block = jnp.concatenate([recv_c[pl.ds(2 * comp + e, 64, stride=8), :] for e in range(2)], 0)
            for a, pair in enumerate(x_forward(block, plain_cos, plain_sin, x_out)):
                at = pl.ds(128 * a, 128)
                keep = mask[:, at].astype(F32) * TIME_STEP
                for i in range(2):
                    out[comp, 0, i, :, at] = out[comp, 0, i, :, at] + pair[i] * keep

    w_send[...] = out[2, 0]

    def w_to_low():
        return pltpu.make_async_remote_copy(
            w_send, w_high, w_sems.at[0], w_sems.at[1], device_id={"gz": plane - 1, "pa": me})

    def w_to_high():
        return pltpu.make_async_remote_copy(
            w_send, w_low, w_sems.at[2], w_sems.at[3], device_id={"gz": plane + 1, "pa": me})

    @pl.when(has_low)
    def _():
        w_to_low().start()

    @pl.when(has_high)
    def _():
        w_to_high().start()

    for a in range(8):
        at = pl.ds(128 * a, 128)
        div[0, 0, :, at] = -(kx(a) * out[0, 0, 1, :, at]) - ky * out[1, 0, 1, :, at]
        div[0, 1, :, at] = kx(a) * out[0, 0, 0, :, at] + ky * out[1, 0, 0, :, at]

    @pl.when(has_low)
    def _():
        pltpu.make_async_copy(w_low, w_low, w_sems.at[3]).wait()

    @pl.when(has_high)
    def _():
        pltpu.make_async_copy(w_high, w_high, w_sems.at[1]).wait()

    div[0] = div[0] + 0.5 * (w_high[...] - w_low[...])

    wait_all(send_a, a_sems.at[0], 8 * (RANKS - 1))
    wait_all(send_b, b_sems.at[0], 4 * (RANKS - 1))

    @pl.when(inside)
    def _():
        wait_all(send_c, c_sems.at[0], 6 * LAST_RANK)

    @pl.when(jnp.logical_not(inside))
    def _():
        wait_all(send_c, c_sems.at[0], 6 * (LAST_RANK + 1))

    @pl.when(has_low)
    def _():
        to_low(0).wait_send()
        to_low(1).wait_send()
        w_to_low().wait_send()

    @pl.when(has_high)
    def _():
        to_high(0).wait_send()
        to_high(1).wait_send()
        w_to_high().wait_send()


def on_device(velocity, mode_mask):
    constants = tables()
    operands = (velocity, mode_mask, *(jnp.asarray(constants[name]) for name in NAMES))
    whole = pl.BlockSpec(memory_space=pltpu.VMEM)
    dma, vmem = pltpu.SemaphoreType.DMA, pltpu.VMEM
    return pl.pallas_call(
        kernel,
        name="substep",
        out_shape=(
            vmem((3, 1, 2, 8, 1024), F32),
            vmem((1, 2, 8, 1024), F32),
        ),
        in_specs=[pl.BlockSpec(memory_space=pl.ANY)] * len(operands),
        out_specs=(whole, whole),
        scratch_shapes=[
            *(vmem(operand.shape, operand.dtype) for operand in operands), dma((len(operands),)),
            vmem((512, 128), F32), vmem((512, 128), F32),
            vmem((256, 128), F32), vmem((256, 128), F32),
            vmem((512, 128), F32), vmem((512, 128), F32),
            vmem((3, 2, 8, 1024), F32), vmem((3, 2, 8, 1024), F32),
            vmem((2, 8, 1024), F32), vmem((2, 8, 1024), F32), vmem((2, 8, 1024), F32),
            dma((2,)), dma((2,)), dma((2,)),
            dma((2,)), dma((2,)), dma((2,)), dma((2,)), dma((4,)),
        ],
        compiler_params=pltpu.CompilerParams(collective_id=0, has_side_effects=True),
    )(*operands)


def solution(mesh):
    return jax.shard_map(
        on_device,
        mesh=mesh,
        in_specs=(P(None, "gz", None, "pa", None), P("pa", None)),
        out_specs=(P(None, "gz", None, "pa", None), P("gz", None, "pa", None)),
        check_vma=False,
    )
```

```python
import math

import jax
import jax.numpy as jnp
import numpy as np
from jax import lax
from jax.experimental import pallas as pl
from jax.experimental.pallas import tpu as pltpu
from jax.sharding import PartitionSpec as P


TWO_PI = 2.0 * math.pi
TIME_STEP = 0.2
VISCOSITY = 0.25
RANKS = 64
WORKERS = 32
LAST_RANK = 42
F32 = jnp.float32
BF16 = jnp.bfloat16


def halves(table):
    table = np.asarray(table, np.float32)
    high = table.astype(jnp.bfloat16)
    low = (table - high.astype(np.float32)).astype(jnp.bfloat16)
    return np.stack([high, low])


def tables():
    index = np.arange
    k, b, c, s, q, r = index(32), index(128), index(8), index(8), index(64), index(128)
    d = (4 * k[None, :] + index(4)[:, None]).reshape(-1)
    angle = TWO_PI / 128.0 * (d[:, None] * b[None, :] % 128)
    cos, sin = np.cos(angle) / 32.0, np.sin(angle) / 32.0
    x_in = np.block([[cos, -sin], [sin, cos]])
    angle = TWO_PI / 1024.0 * (c[:, None] * b[None, :])
    x_turn = np.stack([np.cos(angle), np.sin(angle)]).astype(np.float32).reshape(2, 8, 1, 128)
    angle = TWO_PI / 128.0 * (r[:, None] * q[None, :] % 128)
    cos, sin = np.cos(angle) / 32.0, np.sin(angle) / 32.0
    y_in = np.block([[cos, -sin], [sin, cos]])
    angle = TWO_PI / 1024.0 * (r[:, None] * np.tile(s, 16)[None, :])
    y_turn = np.stack([np.cos(angle), np.sin(angle)]).astype(np.float32)
    angle = TWO_PI / 8.0 * (s[:, None] * s[None, :] % 8)
    cos8, sin8 = np.cos(angle), np.sin(angle)
    eye = np.eye(8)
    real = np.kron(np.eye(2), np.kron(eye, cos8))
    imag = np.kron(np.eye(2), np.kron(eye, -sin8))
    both = np.concatenate([real, imag], 0)
    y_grid = np.concatenate([both, np.roll(both, 64, axis=1)], 1)
    real = np.kron(eye, cos8) / 32.0
    imag = np.kron(eye, -sin8) / 32.0
    line = np.concatenate([real, imag, imag, -real], 1)
    y_low = np.concatenate([line, np.zeros_like(line)], 0)
    y_diff = np.concatenate([line, -line], 0)
    angle = TWO_PI / 128.0 * (q[:, None] * r[None, :] % 128)
    y_out = np.concatenate([np.cos(angle), np.sin(angle)], 1)
    angle = TWO_PI / 128.0 * (d[:, None] * b[None, :] % 128)
    x_out = np.concatenate([np.cos(angle), np.sin(angle)], 1) / 32.0
    return dict(
        x_in=halves(x_in),
        x_turn=x_turn,
        y_in=halves(y_in),
        y_turn=y_turn,
        y_grid=halves(y_grid),
        y_low=halves(y_low),
        y_diff=halves(y_diff),
        y_out=halves(y_out),
        x_out=halves(x_out),
    )


NAMES = ("x_in", "x_turn", "y_in", "y_turn", "y_grid", "y_low", "y_diff", "y_out", "x_out")


def split(value):
    high = value.astype(BF16)
    return high, (value - high.astype(F32)).astype(BF16)


def dot(left, right, contract=((1,), (0,))):
    def one(i, j):
        return lax.dot_general(left[i], right[j], (contract, ((), ())), preferred_element_type=F32)

    return one(0, 0) + (one(0, 1) + one(1, 0))


def eight(values, sign):
    count = len(values)
    if count == 1:
        return values
    even, odd = eight(values[0::2], sign), eight(values[1::2], sign)
    half = count // 2
    low, high = [], []
    for k in range(half):
        (er, ei), (qr, qi) = even[k], odd[k]
        turn = 8 // count * k
        if turn == 0:
            tr, ti = qr, qi
        elif turn == 2:
            tr, ti = -sign * qi, sign * qr
        else:
            root = math.sqrt(0.5)
            if turn == 1:
                tr, ti = root * (qr - sign * qi), root * (qi + sign * qr)
            else:
                tr, ti = -root * (qr + sign * qi), root * (sign * qr - qi)
        low.append((er + tr, ei + ti))
        high.append((er - tr, ei - ti))
    return low + high


def x_inverse(fields, turn_cos, turn_sin, table):
    real, imag = [], []
    for field in fields:
        for c, (vr, vi) in enumerate(eight(field, 1.0)):
            real.append(vr * turn_cos[c] - vi * turn_sin[c])
            imag.append(vr * turn_sin[c] + vi * turn_cos[c])
    lines = jnp.concatenate([jnp.concatenate(real, 0), jnp.concatenate(imag, 0)], 1)
    return dot(table, split(lines), ((1,), (1,)))


def y_turned(modes, cos, sin, table):
    lines = dot(table, split(modes))
    out = []
    for k in range(modes.shape[1] // 128):
        vr, vi = lines[:128, 128 * k : 128 * k + 128], lines[128:, 128 * k : 128 * k + 128]
        out.append(jnp.concatenate([vr * cos - vi * sin, vr * sin + vi * cos], 1))
    return out


def y_forward(product, cos, sin, table):
    line = dot(split(product), table)
    one, two = line[:, :128], line[:, 128:]
    return jnp.concatenate([one * cos + two * sin, two * cos - one * sin], 0)


def x_forward(block, turn_cos, turn_sin, table):
    line = dot(split(block.T), table)
    values = []
    for c in range(8):
        re, im = line[8 * c : 8 * c + 8], line[64 + 8 * c : 72 + 8 * c]
        vr, vi = re[:, :128] + im[:, 128:], im[:, :128] - re[:, 128:]
        values.append((vr * turn_cos[c] + vi * turn_sin[c], vi * turn_cos[c] - vr * turn_sin[c]))
    return eight(values, -1.0)


def step(index):
    return (1 - 2 * lax.rem(index, 2)) * lax.div(index + 1, 2)


def partner(me, index):
    dx = 2 + step(lax.rem(index, 4))
    dy = 4 + step(lax.div(index, 4))
    return lax.rem(lax.div(me, 8) + dy, 8) * 4 + lax.rem(lax.rem(me, 4) + dx, 4)


def rank(place, half):
    return lax.div(place, 4) * 8 + half * 4 + lax.rem(place, 4)


def rows(start, align, count):
    return pl.ds(pl.multiple_of(start * align, align), count)


def kernel(*refs):
    count = 2 + len(NAMES)
    sources, out, div, held = refs[:count], refs[count], refs[count + 1], refs[count + 2 : 2 * count + 2]
    body(sources, held, out, div, *refs[2 * count + 2 :])


def body(sources, held, out, div, load_sems,
           send_a, recv_a, send_b, recv_b, send_c, recv_c, low, high, w_low, w_high, w_send,
           a_sems, b_sems, c_sems, low_send, low_recv, high_send, high_recv, w_sems):
    me, plane = lax.axis_index("pa"), lax.axis_index("gz")
    barrier = pltpu.get_barrier_semaphore()
    vel, mask, x_in, x_turn, y_in, y_turn, y_grid, y_low, y_diff, y_out, x_out = held

    def load(i):
        return pltpu.make_async_copy(sources[i], held[i], load_sems.at[i])

    for i in (0, 2, 3):
        load(i).start()

    half = lax.rem(lax.div(me, 4), 2)
    worker, late = half == 0, half == 1
    place = lax.div(me, 8) * 4 + lax.rem(me, 4)
    has_low, has_high = plane > 0, plane < 7

    def greet(dest):
        pl.semaphore_signal(barrier, inc=1, device_id={"gz": plane, "pa": dest})

    @pl.when(worker)
    def _():
        def hello(i, _):
            spot = partner(me, i)
            greet(rank(spot, 1))
            greet(rank(spot, 0))
            return 0

        lax.fori_loop(0, WORKERS - 1, hello, 0)
        greet(rank(place, 1))

    @pl.when(has_low)
    def _():
        pl.semaphore_signal(barrier, inc=1, device_id={"gz": plane - 1, "pa": me})

    @pl.when(has_high)
    def _():
        pl.semaphore_signal(barrier, inc=1, device_id={"gz": plane + 1, "pa": me})

    rest = [i for i in range(len(held)) if i not in (0, 2, 3)]
    for i in rest:
        load(i).start()
    sub = lax.broadcasted_iota(jnp.int32, (8, 128), 0)
    lane = lax.broadcasted_iota(jnp.int32, (8, 128), 1)
    modes = me * 8 + sub
    ky = (TWO_PI / 1024.0) * modes.astype(F32)
    weight = jnp.where(modes == 0, 1.0, 2.0).astype(F32)

    def kx(a):
        return (TWO_PI / 1024.0) * (lane + (128 * a - 1024 * (a // 4))).astype(F32)

    def piece(ref, *lead):
        return [ref[(*lead, slice(None), pl.ds(128 * a, 128))] for a in range(8)]

    for i in (0, 2, 3):
        load(i).wait()
    turn_cos = [weight * x_turn[0, c] for c in range(8)]
    turn_sin = [weight * x_turn[1, c] for c in range(8)]

    def field(comp):
        return list(zip(piece(vel, comp, 0, 0), piece(vel, comp, 0, 1), strict=True))

    u, v, w = field(0), field(1), field(2)
    omega_z = [
        (ky * u[a][1] - kx(a) * v[a][1], kx(a) * v[a][0] - ky * u[a][0]) for a in range(8)
    ]
    grid = x_inverse([u, v, w, omega_z], turn_cos, turn_sin, x_in)
    for k in range(2):
        for j in range(8):
            send_a[pl.ds(8 * k + j, 32, stride=16), :] = grid[32 * j : 32 * j + 32, 128 * k : 128 * k + 128]

    sides = jnp.where(jnp.logical_and(has_low, has_high), 2, 1)
    pl.semaphore_wait(barrier, WORKERS - 1 + half + sides)

    def to_low(group):
        comps = pl.ds(0, 2) if group == 0 else pl.ds(2, 1)
        return pltpu.make_async_remote_copy(
            vel.at[comps, 0], high.at[comps], low_send.at[group], high_recv.at[group],
            device_id={"gz": plane - 1, "pa": me})

    def to_high(group):
        comps = pl.ds(0, 2) if group == 0 else pl.ds(2, 1)
        return pltpu.make_async_remote_copy(
            vel.at[comps, 0], low.at[comps], high_send.at[group], low_recv.at[group],
            device_id={"gz": plane + 1, "pa": me})

    @pl.when(has_low)
    def _():
        to_low(0).start()

    @pl.when(has_high)
    def _():
        to_high(0).start()

    def send(source, target, sems, align, count, from_spot, to_spot, dest):
        return pltpu.make_async_remote_copy(
            source.at[rows(to_spot, align, count)], target.at[rows(from_spot, align, count)],
            sems.at[0], sems.at[1], device_id={"gz": plane, "pa": dest})

    def to_workers(source, target, sems, count):
        def start(i, _):
            spot = partner(me, i)
            send(source, target, sems, count, count, me, spot, rank(spot, 0)).start()
            return 0

        lax.fori_loop(0, WORKERS - 1, start, 0)

        @pl.when(late)
        def _():
            send(source, target, sems, count, count, me, place, rank(place, 0)).start()

    to_workers(send_a, recv_a, a_sems, 16)

    @pl.when(has_low)
    def _():
        to_low(1).start()
        pltpu.make_async_copy(low.at[pl.ds(0, 2)], low.at[pl.ds(0, 2)], low_recv.at[0]).wait()

    @pl.when(jnp.logical_not(has_low))
    def _():
        low[...] = jnp.zeros_like(low)
        w_low[...] = jnp.zeros_like(w_low)

    @pl.when(has_high)
    def _():
        to_high(1).start()
        pltpu.make_async_copy(high.at[pl.ds(0, 2)], high.at[pl.ds(0, 2)], high_recv.at[0]).wait()

    @pl.when(jnp.logical_not(has_high))
    def _():
        high[...] = jnp.zeros_like(high)
        w_high[...] = jnp.zeros_like(w_high)

    def slope(comp):
        pairs = []
        for a in range(8):
            at = pl.ds(128 * a, 128)
            pairs.append(tuple(0.5 * (high[comp, i, :, at] - low[comp, i, :, at]) for i in range(2)))
        return pairs

    dz_u, dz_v = slope(0), slope(1)
    w = field(2)
    omega_x = [(-(ky * w[a][1]) - dz_v[a][0], ky * w[a][0] - dz_v[a][1]) for a in range(8)]
    omega_y = [(dz_u[a][0] + kx(a) * w[a][1], dz_u[a][1] - kx(a) * w[a][0]) for a in range(8)]
    grid = x_inverse([omega_x, omega_y], turn_cos, turn_sin, x_in)
    for j in range(8):
        send_b[pl.ds(j, 32, stride=8), :] = grid[32 * j : 32 * j + 32]
    to_workers(send_b, recv_b, b_sems, 8)

    def wait_all(ref, sem, count):
        view = ref.at[pl.ds(0, count)]
        pltpu.make_async_copy(view, view, sem).wait()

    for i in rest:
        load(i).wait()
    inside = me <= LAST_RANK

    @pl.when(worker)
    def _():
        recv_a[rows(me, 16, 16), :] = send_a[rows(place, 16, 16), :]
        recv_b[rows(me, 8, 8), :] = send_b[rows(place, 8, 8), :]
        cos, sin = y_turn[0], y_turn[1]

        def gathered(ref, stride, base):
            return jnp.concatenate(
                [ref[pl.ds(base, 64, stride=stride), :], ref[pl.ds(base + 4, 64, stride=stride), :]], 0)

        def on_grid(ref, stride, bases):
            turned = y_turned(jnp.concatenate([gathered(ref, stride, base) for base in bases], 1), cos, sin, y_in)
            return [dot(split(value), y_grid) for value in turned]

        wait_all(recv_a, a_sems.at[1], 16 * (RANKS - 1))
        first = on_grid(recv_a, 16, [8 * k + e for k in range(2) for e in range(4)])
        wait_all(recv_b, b_sems.at[1], 8 * (RANKS - 1))
        second = on_grid(recv_b, 8, range(4))

        products = [[], [], []]
        for e in range(4):
            uv, wz, xy = first[e], first[4 + e], second[e]
            uv, vu = uv[:, :128], uv[:, 128:]
            wz, zw = wz[:, :128], wz[:, 128:]
            xy, yx = xy[:, :128], xy[:, 128:]
            products[0].append(vu * zw - wz * yx)
            products[1].append(wz * xy - uv * zw)
            products[2].append(uv * yx)
        for comp in range(3):
            table = y_diff if comp == 2 else y_low
            lines = [y_forward(value, cos, sin, table) for value in products[comp]]
            spectral = dot(y_out, split(jnp.concatenate(lines, 1)))
            for e in range(4):
                send_c[pl.ds(4 * comp + e, 64, stride=16), :] = spectral[:, 128 * e : 128 * e + 128]

        def start_c(spot, to_half):
            dest = rank(spot, to_half)

            @pl.when(dest <= LAST_RANK)
            def _():
                send(send_c, recv_c, c_sems, 16, 12, place, dest, dest).start()

        for to_half in range(2):
            def start(i, _):
                start_c(partner(me, i), to_half)
                return 0

            lax.fori_loop(0, WORKERS - 1, start, 0)
        start_c(place, 1)

        @pl.when(inside)
        def _():
            recv_c[rows(place, 16, 12), :] = send_c[rows(me, 16, 12), :]

    @pl.when(has_low)
    def _():
        pltpu.make_async_copy(low.at[pl.ds(2, 1)], low.at[pl.ds(2, 1)], low_recv.at[1]).wait()

    @pl.when(has_high)
    def _():
        pltpu.make_async_copy(high.at[pl.ds(2, 1)], high.at[pl.ds(2, 1)], high_recv.at[1]).wait()

    for comp in range(3):
        for i in range(2):
            for a in range(8):
                at = pl.ds(128 * a, 128)
                mid = vel[comp, 0, i, :, at]
                viscous = (high[comp, i, :, at] - 2.0 * mid + low[comp, i, :, at]) - (kx(a) * kx(a) + ky * ky) * mid
                out[comp, 0, i, :, at] = mid + (TIME_STEP * VISCOSITY) * viscous

    @pl.when(inside)
    def _():
        @pl.when(worker)
        def _():
            wait_all(recv_c, c_sems.at[1], 12 * (WORKERS - 1))

        @pl.when(late)
        def _():
            wait_all(recv_c, c_sems.at[1], 12 * WORKERS)

        plain_cos = [jnp.broadcast_to(x_turn[0, c], (8, 128)) for c in range(8)]
        plain_sin = [jnp.broadcast_to(x_turn[1, c], (8, 128)) for c in range(8)]
        for comp in range(3):
            block = jnp.concatenate([recv_c[pl.ds(4 * comp + e, 32, stride=16), :] for e in range(4)], 0)
            for a, pair in enumerate(x_forward(block, plain_cos, plain_sin, x_out)):
                at = pl.ds(128 * a, 128)
                keep = mask[:, at].astype(F32) * TIME_STEP
                for i in range(2):
                    out[comp, 0, i, :, at] = out[comp, 0, i, :, at] + pair[i] * keep

    w_send[...] = out[2, 0]

    def w_to_low():
        return pltpu.make_async_remote_copy(
            w_send, w_high, w_sems.at[0], w_sems.at[1], device_id={"gz": plane - 1, "pa": me})

    def w_to_high():
        return pltpu.make_async_remote_copy(
            w_send, w_low, w_sems.at[2], w_sems.at[3], device_id={"gz": plane + 1, "pa": me})

    @pl.when(has_low)
    def _():
        w_to_low().start()

    @pl.when(has_high)
    def _():
        w_to_high().start()

    for a in range(8):
        at = pl.ds(128 * a, 128)
        div[0, 0, :, at] = -(kx(a) * out[0, 0, 1, :, at]) - ky * out[1, 0, 1, :, at]
        div[0, 1, :, at] = kx(a) * out[0, 0, 0, :, at] + ky * out[1, 0, 0, :, at]

    @pl.when(has_low)
    def _():
        pltpu.make_async_copy(w_low, w_low, w_sems.at[3]).wait()

    @pl.when(has_high)
    def _():
        pltpu.make_async_copy(w_high, w_high, w_sems.at[1]).wait()

    div[0] = div[0] + 0.5 * (w_high[...] - w_low[...])

    def all_left(times):
        wait_all(send_a, a_sems.at[0], 16 * times)
        wait_all(send_b, b_sems.at[0], 8 * times)

    @pl.when(worker)
    def _():
        all_left(WORKERS - 1)

        @pl.when(inside)
        def _():
            wait_all(send_c, c_sems.at[0], 12 * LAST_RANK)

        @pl.when(jnp.logical_not(inside))
        def _():
            wait_all(send_c, c_sems.at[0], 12 * (LAST_RANK + 1))

    @pl.when(late)
    def _():
        all_left(WORKERS)

    @pl.when(has_low)
    def _():
        to_low(0).wait_send()
        to_low(1).wait_send()
        w_to_low().wait_send()

    @pl.when(has_high)
    def _():
        to_high(0).wait_send()
        to_high(1).wait_send()
        w_to_high().wait_send()


def on_device(velocity, mode_mask):
    constants = tables()
    operands = (velocity, mode_mask, *(jnp.asarray(constants[name]) for name in NAMES))
    whole = pl.BlockSpec(memory_space=pltpu.VMEM)
    dma, vmem = pltpu.SemaphoreType.DMA, pltpu.VMEM
    return pl.pallas_call(
        kernel,
        name="substep",
        out_shape=(
            vmem((3, 1, 2, 8, 1024), F32),
            vmem((1, 2, 8, 1024), F32),
        ),
        in_specs=[pl.BlockSpec(memory_space=pl.ANY)] * len(operands),
        out_specs=(whole, whole),
        scratch_shapes=[
            *(vmem(operand.shape, operand.dtype) for operand in operands), dma((len(operands),)),
            vmem((512, 128), F32), vmem((1024, 128), F32),
            vmem((256, 128), F32), vmem((512, 128), F32),
            vmem((1024, 128), F32), vmem((512, 128), F32),
            vmem((3, 2, 8, 1024), F32), vmem((3, 2, 8, 1024), F32),
            vmem((2, 8, 1024), F32), vmem((2, 8, 1024), F32), vmem((2, 8, 1024), F32),
            dma((2,)), dma((2,)), dma((2,)),
            dma((2,)), dma((2,)), dma((2,)), dma((2,)), dma((4,)),
        ],
        compiler_params=pltpu.CompilerParams(collective_id=0, has_side_effects=True),
    )(*operands)


def solution(mesh):
    return jax.shard_map(
        on_device,
        mesh=mesh,
        in_specs=(P(None, "gz", None, "pa", None), P("pa", None)),
        out_specs=(P(None, "gz", None, "pa", None), P("gz", None, "pa", None)),
        check_vma=False,
    )
```

```python
import math

import jax
import jax.numpy as jnp
import numpy as np
from jax import lax
from jax.experimental import pallas as pl
from jax.experimental.pallas import tpu as pltpu
from jax.sharding import PartitionSpec as P


TWO_PI = 2.0 * math.pi
TIME_STEP = 0.2
VISCOSITY = 0.25
RANKS = 64
LAST_RANK = 42
F32 = jnp.float32
BF16 = jnp.bfloat16


def halves(table):
    table = np.asarray(table, np.float32)
    high = table.astype(jnp.bfloat16)
    low = (table - high.astype(np.float32)).astype(jnp.bfloat16)
    return np.stack([high, low])


def tables():
    index = np.arange
    p, b, c, s, q, r = index(64), index(128), index(8), index(8), index(64), index(128)
    d = (2 * p[None, :] + index(2)[:, None]).reshape(-1)
    angle = TWO_PI / 128.0 * (d[:, None] * b[None, :] % 128)
    cos, sin = np.cos(angle) / 32.0, np.sin(angle) / 32.0
    x_in = np.block([[cos, -sin], [sin, cos]])
    angle = TWO_PI / 1024.0 * (c[:, None] * b[None, :])
    x_turn = np.stack([np.cos(angle), np.sin(angle)]).astype(np.float32).reshape(2, 8, 1, 128)
    angle = TWO_PI / 128.0 * (r[:, None] * q[None, :] % 128)
    cos, sin = np.cos(angle) / 32.0, np.sin(angle) / 32.0
    y_in = np.block([[cos, -sin], [sin, cos]])
    angle = TWO_PI / 1024.0 * (r[:, None] * np.tile(s, 16)[None, :])
    y_turn = np.stack([np.cos(angle), np.sin(angle)]).astype(np.float32)
    angle = TWO_PI / 8.0 * (s[:, None] * s[None, :] % 8)
    cos8, sin8 = np.cos(angle), np.sin(angle)
    eye = np.eye(8)
    real = np.kron(np.eye(2), np.kron(eye, cos8))
    imag = np.kron(np.eye(2), np.kron(eye, -sin8))
    both = np.concatenate([real, imag], 0)
    y_grid = np.concatenate([both, np.roll(both, 64, axis=1)], 1)
    real = np.kron(eye, cos8) / 32.0
    imag = np.kron(eye, -sin8) / 32.0
    line = np.concatenate([real, imag, imag, -real], 1)
    y_low = np.concatenate([line, np.zeros_like(line)], 0)
    y_diff = np.concatenate([line, -line], 0)
    angle = TWO_PI / 128.0 * (q[:, None] * r[None, :] % 128)
    y_out = np.concatenate([np.cos(angle), np.sin(angle)], 1)
    angle = TWO_PI / 128.0 * (d[:, None] * b[None, :] % 128)
    x_out = np.concatenate([np.cos(angle), np.sin(angle)], 1) / 32.0
    return dict(
        x_in=halves(x_in),
        x_turn=x_turn,
        y_in=halves(y_in),
        y_turn=y_turn,
        y_grid=halves(y_grid),
        y_low=halves(y_low),
        y_diff=halves(y_diff),
        y_out=halves(y_out),
        x_out=halves(x_out),
    )


NAMES = ("x_in", "x_turn", "y_in", "y_turn", "y_grid", "y_low", "y_diff", "y_out", "x_out")


def split(value):
    high = value.astype(BF16)
    return high, (value - high.astype(F32)).astype(BF16)


def dot(left, right, contract=((1,), (0,))):
    def one(i, j):
        return lax.dot_general(left[i], right[j], (contract, ((), ())), preferred_element_type=F32)

    return one(0, 0) + (one(0, 1) + one(1, 0))


def eight(values, sign):
    count = len(values)
    if count == 1:
        return values
    even, odd = eight(values[0::2], sign), eight(values[1::2], sign)
    half = count // 2
    low, high = [], []
    for k in range(half):
        (er, ei), (qr, qi) = even[k], odd[k]
        turn = 8 // count * k
        if turn == 0:
            tr, ti = qr, qi
        elif turn == 2:
            tr, ti = -sign * qi, sign * qr
        else:
            root = math.sqrt(0.5)
            if turn == 1:
                tr, ti = root * (qr - sign * qi), root * (qi + sign * qr)
            else:
                tr, ti = -root * (qr + sign * qi), root * (sign * qr - qi)
        low.append((er + tr, ei + ti))
        high.append((er - tr, ei - ti))
    return low + high


def x_inverse(fields, turn_cos, turn_sin, table):
    real, imag = [], []
    for field in fields:
        for c, (vr, vi) in enumerate(eight(field, 1.0)):
            real.append(vr * turn_cos[c] - vi * turn_sin[c])
            imag.append(vr * turn_sin[c] + vi * turn_cos[c])
    lines = jnp.concatenate([jnp.concatenate(real, 0), jnp.concatenate(imag, 0)], 1)
    return dot(table, split(lines), ((1,), (1,)))


def y_turned(modes, cos, sin, table):
    lines = dot(table, split(modes))
    out = []
    for k in range(modes.shape[1] // 128):
        vr, vi = lines[:128, 128 * k : 128 * k + 128], lines[128:, 128 * k : 128 * k + 128]
        out.append(jnp.concatenate([vr * cos - vi * sin, vr * sin + vi * cos], 1))
    return out


def y_forward(product, cos, sin, table):
    line = dot(split(product), table)
    one, two = line[:, :128], line[:, 128:]
    return jnp.concatenate([one * cos + two * sin, two * cos - one * sin], 0)


def x_forward(block, turn_cos, turn_sin, table):
    line = dot(split(block.T), table)
    values = []
    for c in range(8):
        re, im = line[8 * c : 8 * c + 8], line[64 + 8 * c : 72 + 8 * c]
        vr, vi = re[:, :128] + im[:, 128:], im[:, :128] - re[:, 128:]
        values.append((vr * turn_cos[c] + vi * turn_sin[c], vi * turn_cos[c] - vr * turn_sin[c]))
    return eight(values, -1.0)


HOPS = [(dy, dz, dx) for dy in (4, 3, 5, 2, 6, 1, 7, 0) for dx in (2, 1, 3, 0) for dz in (1, 0)][:-1]


def partners(me):
    x, z, y = lax.rem(me, 4), lax.rem(lax.div(me, 4), 2), lax.div(me, 8)
    xs = [lax.rem(x + i, 4) for i in range(4)]
    zs = [4 * lax.rem(z + i, 2) for i in range(2)]
    ys = [8 * lax.rem(y + i, 8) for i in range(8)]
    return [ys[dy] + zs[dz] + xs[dx] for dy, dz, dx in HOPS]


def rows(start, align, count):
    return pl.ds(pl.multiple_of(start * align, align), count)


def kernel(*refs):
    count = 2 + len(NAMES)
    sources, out, div, held = refs[:count], refs[count], refs[count + 1], refs[count + 2 : 2 * count + 2]
    body(sources, held, out, div, *refs[2 * count + 2 :])


def body(sources, held, out, div, load_sems,
           send_a, recv_a, send_w, recv_w, send_c, recv_c, uv_send, uv_low, uv_high,
           low, high, w_low, w_high, w_send, a_sems, hz_sems, c_sems, uv_sems, halo_sems, w_sems):
    me, plane = lax.axis_index("pa"), lax.axis_index("gz")
    barrier = pltpu.get_barrier_semaphore()
    vel, mask, x_in, x_turn, y_in, y_turn, y_grid, y_low, y_diff, y_out, x_out = held

    def load(i):
        return pltpu.make_async_copy(sources[i], held[i], load_sems.at[i])

    for i in (0, 2, 3):
        load(i).start()

    others = partners(me)
    for other in others:
        pl.semaphore_signal(barrier, inc=1, device_id={"gz": plane, "pa": other})
    has_low, has_high = plane > 0, plane < 7

    @pl.when(has_low)
    def _():
        pl.semaphore_signal(barrier, inc=1, device_id={"gz": plane - 1, "pa": me})

    @pl.when(has_high)
    def _():
        pl.semaphore_signal(barrier, inc=1, device_id={"gz": plane + 1, "pa": me})

    rest = [i for i in range(len(held)) if i not in (0, 2, 3)]
    for i in rest:
        load(i).start()
    sub = lax.broadcasted_iota(jnp.int32, (8, 128), 0)
    lane = lax.broadcasted_iota(jnp.int32, (8, 128), 1)
    modes = me * 8 + sub
    ky = (TWO_PI / 1024.0) * modes.astype(F32)
    weight = jnp.where(modes == 0, 1.0, 2.0).astype(F32)

    def kx(a):
        return (TWO_PI / 1024.0) * (lane + (128 * a - 1024 * (a // 4))).astype(F32)

    def piece(ref, *lead):
        return [ref[(*lead, slice(None), pl.ds(128 * a, 128))] for a in range(8)]

    for i in (0, 2, 3):
        load(i).wait()
    turn_cos = [weight * x_turn[0, c] for c in range(8)]
    turn_sin = [weight * x_turn[1, c] for c in range(8)]

    def field(comp):
        return list(zip(piece(vel, comp, 0, 0), piece(vel, comp, 0, 1), strict=True))

    u, v, w = field(0), field(1), field(2)
    omega_z = [
        (ky * u[a][1] - kx(a) * v[a][1], kx(a) * v[a][0] - ky * u[a][0]) for a in range(8)
    ]
    curl_x = [(-(ky * w[a][1]), ky * w[a][0]) for a in range(8)]
    curl_y = [(kx(a) * w[a][1], -(kx(a) * w[a][0])) for a in range(8)]
    grid = x_inverse([u, v, w, omega_z, curl_x, curl_y], turn_cos, turn_sin, x_in)
    for k in range(3):
        for j in range(4):
            send_a[pl.ds(4 * k + j, 64, stride=16), :] = grid[64 * j : 64 * j + 64, 128 * k : 128 * k + 128]

    @pl.when(jnp.logical_and(has_low, has_high))
    def _():
        pl.semaphore_wait(barrier, RANKS + 1)

    @pl.when(jnp.logical_not(jnp.logical_and(has_low, has_high)))
    def _():
        pl.semaphore_wait(barrier, RANKS)

    def send(source, target, sems, align, count, dest):
        return pltpu.make_async_remote_copy(
            source.at[rows(dest, align, count)], target.at[rows(me, align, count)],
            sems.at[0], sems.at[1], device_id={"gz": plane, "pa": dest})

    for other in others:
        send(send_a, recv_a, a_sems, 16, 12, other).start()

    def beside(source, target_low, target_high, sems):
        down = pltpu.make_async_remote_copy(
            source, target_high, sems.at[0], sems.at[1], device_id={"gz": plane - 1, "pa": me})
        up = pltpu.make_async_remote_copy(
            source, target_low, sems.at[2], sems.at[3], device_id={"gz": plane + 1, "pa": me})
        return down, up

    def start_beside(pair):
        @pl.when(has_low)
        def _():
            pair[0].start()

        @pl.when(has_high)
        def _():
            pair[1].start()

    def from_beside(pair):
        @pl.when(has_low)
        def _():
            pair[1].wait_recv()

        @pl.when(has_high)
        def _():
            pair[0].wait_recv()

    def left_beside(pair):
        @pl.when(has_low)
        def _():
            pair[0].wait_send()

        @pl.when(has_high)
        def _():
            pair[1].wait_send()

    halo = beside(vel.at[:, 0], low, high, halo_sems)
    uv_halo = beside(uv_send, uv_low, uv_high, uv_sems)
    w_halo = beside(w_send, w_low, w_high, w_sems)
    start_beside(halo)

    @pl.when(jnp.logical_not(has_low))
    def _():
        low[...] = jnp.zeros_like(low)
        uv_low[...] = jnp.zeros_like(uv_low)
        w_low[...] = jnp.zeros_like(w_low)

    @pl.when(jnp.logical_not(has_high))
    def _():
        high[...] = jnp.zeros_like(high)
        uv_high[...] = jnp.zeros_like(uv_high)
        w_high[...] = jnp.zeros_like(w_high)

    recv_a[rows(me, 16, 12), :] = send_a[rows(me, 16, 12), :]

    def wait_all(ref, sem, count):
        view = ref.at[pl.ds(0, count)]
        pltpu.make_async_copy(view, view, sem).wait()

    for i in rest:
        load(i).wait()
    cos, sin = y_turn[0], y_turn[1]
    wait_all(recv_a, a_sems.at[1], 12 * (RANKS - 1))

    def gathered(base):
        return jnp.concatenate(
            [recv_a[pl.ds(base, 64, stride=16), :], recv_a[pl.ds(base + 2, 64, stride=16), :]], 0)

    def on_grid(pairs):
        turned = y_turned(
            jnp.concatenate([gathered(4 * k + e) for k in pairs for e in range(2)], 1), cos, sin, y_in)
        return [dot(split(value), y_grid) for value in turned]

    fields = on_grid((0,))
    for e in range(2):
        uv_send[e] = fields[e][:, :128]
    start_beside(uv_halo)
    fields = fields + on_grid((1, 2))
    from_beside(uv_halo)

    def last(parts):
        return dot(y_out, split(jnp.concatenate(parts, 1)))

    sign = jnp.where(lax.broadcasted_iota(jnp.int32, (128, 128), 1) < 64, 0.5, -0.5).astype(F32)
    products = [[], [], []]
    for e in range(2):
        uv, wz, xy = fields[e], fields[2 + e], fields[4 + e]
        uv, vu = uv[:, :128], uv[:, 128:]
        wz, zw = wz[:, :128], wz[:, 128:]
        slope = sign * (uv_high[e] - uv_low[e])
        xy, yx = xy[:, :128] + pltpu.roll(slope, 64, 1), xy[:, 128:] + slope
        products[0].append(vu * zw - wz * yx)
        products[1].append(wz * xy - uv * zw)
        products[2].append(uv * yx)

    def spectral(comp):
        table = y_diff if comp == 2 else y_low
        return last([y_forward(value, cos, sin, table) for value in products[comp]])

    def to_inside(source, target, sems, count):
        for other in others:
            @pl.when(other <= LAST_RANK)
            def _(other=other):
                send(source, target, sems, count, count, other).start()

    modes_w = spectral(2)
    for e in range(2):
        send_w[pl.ds(e, 64, stride=2), :] = modes_w[:, 128 * e : 128 * e + 128]
    to_inside(send_w, recv_w, hz_sems, 2)
    for comp in range(2):
        modes_c = spectral(comp)
        for e in range(2):
            send_c[pl.ds(2 * comp + e, 64, stride=4), :] = modes_c[:, 128 * e : 128 * e + 128]
    to_inside(send_c, recv_c, c_sems, 4)

    inside = me <= LAST_RANK

    from_beside(halo)

    for comp in range(3):
        for i in range(2):
            for a in range(8):
                at = pl.ds(128 * a, 128)
                mid = vel[comp, 0, i, :, at]
                viscous = (high[comp, i, :, at] - 2.0 * mid + low[comp, i, :, at]) - (kx(a) * kx(a) + ky * ky) * mid
                out[comp, 0, i, :, at] = mid + (TIME_STEP * VISCOSITY) * viscous

    plain_cos = [jnp.broadcast_to(x_turn[0, c], (8, 128)) for c in range(8)]
    plain_sin = [jnp.broadcast_to(x_turn[1, c], (8, 128)) for c in range(8)]

    def add_nonlinear(comp, ref, base, stride):
        block = jnp.concatenate([ref[pl.ds(base + e, 64, stride=stride), :] for e in range(2)], 0)
        for a, pair in enumerate(x_forward(block, plain_cos, plain_sin, x_out)):
            at = pl.ds(128 * a, 128)
            keep = mask[:, at].astype(F32) * TIME_STEP
            for i in range(2):
                out[comp, 0, i, :, at] = out[comp, 0, i, :, at] + pair[i] * keep

    @pl.when(inside)
    def _():
        recv_w[rows(me, 2, 2), :] = send_w[rows(me, 2, 2), :]
        recv_c[rows(me, 4, 4), :] = send_c[rows(me, 4, 4), :]
        wait_all(recv_w, hz_sems.at[1], 2 * (RANKS - 1))
        add_nonlinear(2, recv_w, 0, 2)

    w_send[...] = out[2, 0]
    start_beside(w_halo)

    @pl.when(inside)
    def _():
        wait_all(recv_c, c_sems.at[1], 4 * (RANKS - 1))
        add_nonlinear(0, recv_c, 0, 4)
        add_nonlinear(1, recv_c, 2, 4)

    for a in range(8):
        at = pl.ds(128 * a, 128)
        div[0, 0, :, at] = -(kx(a) * out[0, 0, 1, :, at]) - ky * out[1, 0, 1, :, at]
        div[0, 1, :, at] = kx(a) * out[0, 0, 0, :, at] + ky * out[1, 0, 0, :, at]

    from_beside(w_halo)
    div[0] = div[0] + 0.5 * (w_high[...] - w_low[...])

    wait_all(send_a, a_sems.at[0], 12 * (RANKS - 1))

    @pl.when(inside)
    def _():
        wait_all(send_w, hz_sems.at[0], 2 * LAST_RANK)
        wait_all(send_c, c_sems.at[0], 4 * LAST_RANK)

    @pl.when(jnp.logical_not(inside))
    def _():
        wait_all(send_w, hz_sems.at[0], 2 * (LAST_RANK + 1))
        wait_all(send_c, c_sems.at[0], 4 * (LAST_RANK + 1))

    for pair in (halo, uv_halo, w_halo):
        left_beside(pair)


def on_device(velocity, mode_mask):
    constants = tables()
    operands = (velocity, mode_mask, *(jnp.asarray(constants[name]) for name in NAMES))
    whole = pl.BlockSpec(memory_space=pltpu.VMEM)
    dma, vmem = pltpu.SemaphoreType.DMA, pltpu.VMEM
    return pl.pallas_call(
        kernel,
        name="substep",
        out_shape=(
            vmem((3, 1, 2, 8, 1024), F32),
            vmem((1, 2, 8, 1024), F32),
        ),
        in_specs=[pl.BlockSpec(memory_space=pl.ANY)] * len(operands),
        out_specs=(whole, whole),
        scratch_shapes=[
            *(vmem(operand.shape, operand.dtype) for operand in operands), dma((len(operands),)),
            vmem((1024, 128), F32), vmem((1024, 128), F32),
            vmem((128, 128), F32), vmem((128, 128), F32),
            vmem((256, 128), F32), vmem((256, 128), F32),
            *[vmem((2, 128, 128), F32)] * 3,
            *[vmem((3, 2, 8, 1024), F32)] * 2,
            *[vmem((2, 8, 1024), F32)] * 3,
            *[dma((2,))] * 3, *[dma((4,))] * 3,
        ],
        compiler_params=pltpu.CompilerParams(collective_id=0, has_side_effects=True),
    )(*operands)


def solution(mesh):
    return jax.shard_map(
        on_device,
        mesh=mesh,
        in_specs=(P(None, "gz", None, "pa", None), P("pa", None)),
        out_specs=(P(None, "gz", None, "pa", None), P("gz", None, "pa", None)),
        check_vma=False,
    )
```

```python
import math

import jax
import jax.numpy as jnp
import numpy as np
from jax import lax
from jax.experimental import pallas as pl
from jax.experimental.pallas import tpu as pltpu
from jax.sharding import PartitionSpec as P


TWO_PI = 2.0 * math.pi
TIME_STEP = 0.2
VISCOSITY = 0.25
RANKS = 64
LAST_RANK = 42
F32 = jnp.float32
BF16 = jnp.bfloat16


def halves(table):
    table = np.asarray(table, np.float32)
    high = table.astype(jnp.bfloat16)
    low = (table - high.astype(np.float32)).astype(jnp.bfloat16)
    return np.stack([high, low])


def tables():
    index = np.arange
    p, b, c, s, q, r = index(64), index(128), index(8), index(8), index(64), index(128)
    d = (2 * p[None, :] + index(2)[:, None]).reshape(-1)
    angle = TWO_PI / 128.0 * (d[:, None] * b[None, :] % 128)
    cos, sin = np.cos(angle) / 32.0, np.sin(angle) / 32.0
    x_in = np.block([[cos, -sin], [sin, cos]])
    angle = TWO_PI / 1024.0 * (c[:, None] * b[None, :])
    x_turn = np.stack([np.cos(angle), np.sin(angle)]).astype(np.float32).reshape(2, 8, 1, 128)
    angle = TWO_PI / 128.0 * (r[:, None] * q[None, :] % 128)
    cos, sin = np.cos(angle) / 32.0, np.sin(angle) / 32.0
    y_in = np.block([[cos, -sin], [sin, cos]])
    angle = TWO_PI / 1024.0 * (r[:, None] * np.tile(s, 16)[None, :])
    y_turn = np.stack([np.cos(angle), np.sin(angle)]).astype(np.float32)
    angle = TWO_PI / 8.0 * (s[:, None] * s[None, :] % 8)
    cos8, sin8 = np.cos(angle), np.sin(angle)
    eye = np.eye(8)
    real = np.kron(np.eye(2), np.kron(eye, cos8))
    imag = np.kron(np.eye(2), np.kron(eye, -sin8))
    both = np.concatenate([real, imag], 0)
    y_grid = np.concatenate([both, np.roll(both, 64, axis=1)], 1)
    real = np.kron(eye, cos8) / 32.0
    imag = np.kron(eye, -sin8) / 32.0
    line = np.concatenate([real, imag, imag, -real], 1)
    y_low = np.concatenate([line, np.zeros_like(line)], 0)
    y_diff = np.concatenate([line, -line], 0)
    angle = TWO_PI / 128.0 * (q[:, None] * r[None, :] % 128)
    y_out = np.concatenate([np.cos(angle), np.sin(angle)], 1)
    angle = TWO_PI / 128.0 * (d[:, None] * b[None, :] % 128)
    x_out = np.concatenate([np.cos(angle), np.sin(angle)], 1) / 32.0
    return dict(
        x_in=halves(x_in),
        x_turn=x_turn,
        y_in=halves(y_in),
        y_turn=y_turn,
        y_grid=halves(y_grid),
        y_low=halves(y_low),
        y_diff=halves(y_diff),
        y_out=halves(y_out),
        x_out=halves(x_out),
    )


NAMES = ("x_in", "x_turn", "y_in", "y_turn", "y_grid", "y_low", "y_diff", "y_out", "x_out")


def split(value):
    high = value.astype(BF16)
    return high, (value - high.astype(F32)).astype(BF16)


def dot(left, right, contract=((1,), (0,))):
    def one(i, j):
        return lax.dot_general(left[i], right[j], (contract, ((), ())), preferred_element_type=F32)

    return one(0, 0) + (one(0, 1) + one(1, 0))


def eight(values, sign):
    count = len(values)
    if count == 1:
        return values
    even, odd = eight(values[0::2], sign), eight(values[1::2], sign)
    half = count // 2
    low, high = [], []
    for k in range(half):
        (er, ei), (qr, qi) = even[k], odd[k]
        turn = 8 // count * k
        if turn == 0:
            tr, ti = qr, qi
        elif turn == 2:
            tr, ti = -sign * qi, sign * qr
        else:
            root = math.sqrt(0.5)
            if turn == 1:
                tr, ti = root * (qr - sign * qi), root * (qi + sign * qr)
            else:
                tr, ti = -root * (qr + sign * qi), root * (sign * qr - qi)
        low.append((er + tr, ei + ti))
        high.append((er - tr, ei - ti))
    return low + high


def x_inverse(fields, turn_cos, turn_sin, table):
    real, imag = [], []
    for field in fields:
        for c, (vr, vi) in enumerate(eight(field, 1.0)):
            real.append(vr * turn_cos[c] - vi * turn_sin[c])
            imag.append(vr * turn_sin[c] + vi * turn_cos[c])
    lines = jnp.concatenate([jnp.concatenate(real, 0), jnp.concatenate(imag, 0)], 1)
    return dot(table, split(lines), ((1,), (1,)))


def y_turned(modes, cos, sin, table):
    lines = dot(table, split(modes))
    out = []
    for k in range(modes.shape[1] // 128):
        vr, vi = lines[:128, 128 * k : 128 * k + 128], lines[128:, 128 * k : 128 * k + 128]
        out.append(jnp.concatenate([vr * cos - vi * sin, vr * sin + vi * cos], 1))
    return out


def y_forward(product, cos, sin, table):
    line = dot(split(product), table)
    one, two = line[:, :128], line[:, 128:]
    return jnp.concatenate([one * cos + two * sin, two * cos - one * sin], 0)


def x_forward(block, turn_cos, turn_sin, table):
    line = dot(split(block.T), table)
    values = []
    for c in range(8):
        re, im = line[8 * c : 8 * c + 8], line[64 + 8 * c : 72 + 8 * c]
        vr, vi = re[:, :128] + im[:, 128:], im[:, :128] - re[:, 128:]
        values.append((vr * turn_cos[c] + vi * turn_sin[c], vi * turn_cos[c] - vr * turn_sin[c]))
    return eight(values, -1.0)


HOPS = [(dy, dz, dx) for dz in (1, 0) for dy in (4, 3, 5, 2, 6, 1, 7, 0) for dx in (2, 1, 3, 0)][:-1]


def partners(me):
    x, z, y = lax.rem(me, 4), lax.rem(lax.div(me, 4), 2), lax.div(me, 8)
    xs = [lax.rem(x + i, 4) for i in range(4)]
    zs = [4 * lax.rem(z + i, 2) for i in range(2)]
    ys = [8 * lax.rem(y + i, 8) for i in range(8)]
    return [ys[dy] + zs[dz] + xs[dx] for dy, dz, dx in HOPS]


def rows(start, align, count):
    return pl.ds(pl.multiple_of(start * align, align), count)


def kernel(*refs):
    count = 2 + len(NAMES)
    sources, out, div, held = refs[:count], refs[count], refs[count + 1], refs[count + 2 : 2 * count + 2]
    body(sources, held, out, div, *refs[2 * count + 2 :])


def body(sources, held, out, div, load_sems,
           send_u, recv_u, send_a, recv_a, send_w, recv_w, send_c, recv_c, uv_send, uv_low, uv_high,
           low, high, w_low, w_high, w_send, u_sems, a_sems, hz_sems, c_sems, uv_sems, halo_sems, w_sems):
    me, plane = lax.axis_index("pa"), lax.axis_index("gz")
    barrier = pltpu.get_barrier_semaphore()
    vel, mask, x_in, x_turn, y_in, y_turn, y_grid, y_low, y_diff, y_out, x_out = held

    def load(i):
        return pltpu.make_async_copy(sources[i], held[i], load_sems.at[i])

    for i in (0, 2, 3):
        load(i).start()

    others = partners(me)
    for other in others:
        pl.semaphore_signal(barrier, inc=1, device_id={"gz": plane, "pa": other})
    has_low, has_high = plane > 0, plane < 7

    @pl.when(has_low)
    def _():
        pl.semaphore_signal(barrier, inc=1, device_id={"gz": plane - 1, "pa": me})

    @pl.when(has_high)
    def _():
        pl.semaphore_signal(barrier, inc=1, device_id={"gz": plane + 1, "pa": me})

    rest = [i for i in range(len(held)) if i not in (0, 2, 3)]
    for i in rest:
        load(i).start()
    sub = lax.broadcasted_iota(jnp.int32, (8, 128), 0)
    lane = lax.broadcasted_iota(jnp.int32, (8, 128), 1)
    modes = me * 8 + sub
    ky = (TWO_PI / 1024.0) * modes.astype(F32)
    weight = jnp.where(modes == 0, 1.0, 2.0).astype(F32)

    def kx(a):
        return (TWO_PI / 1024.0) * (lane + (128 * a - 1024 * (a // 4))).astype(F32)

    def piece(ref, *lead):
        return [ref[(*lead, slice(None), pl.ds(128 * a, 128))] for a in range(8)]

    for i in (0, 2, 3):
        load(i).wait()
    turn_cos = [weight * x_turn[0, c] for c in range(8)]
    turn_sin = [weight * x_turn[1, c] for c in range(8)]

    def field(comp):
        return list(zip(piece(vel, comp, 0, 0), piece(vel, comp, 0, 1), strict=True))

    u, v, w = field(0), field(1), field(2)
    omega_z = [
        (ky * u[a][1] - kx(a) * v[a][1], kx(a) * v[a][0] - ky * u[a][0]) for a in range(8)
    ]
    curl_y = [(kx(a) * w[a][1], -(kx(a) * w[a][0])) for a in range(8)]
    grid = x_inverse([u, v, w, omega_z, curl_y, curl_y], turn_cos, turn_sin, x_in)
    left = lax.broadcasted_iota(jnp.int32, (64, 128), 1) < 64
    for j in range(4):
        send_u[pl.ds(j, 64, stride=4), :] = grid[64 * j : 64 * j + 64, :128]
        send_a[pl.ds(j, 64, stride=8), :] = grid[64 * j : 64 * j + 64, 128:256]
    for ri in range(2):
        first, second = (grid[128 * ri + 64 * e : 128 * ri + 64 * e + 64, 256:] for e in range(2))
        send_a[pl.ds(4 + ri, 64, stride=8), :] = jnp.where(left, second, first)

    @pl.when(jnp.logical_and(has_low, has_high))
    def _():
        pl.semaphore_wait(barrier, RANKS + 1)

    @pl.when(jnp.logical_not(jnp.logical_and(has_low, has_high)))
    def _():
        pl.semaphore_wait(barrier, RANKS)

    def send(source, target, sems, align, count, dest):
        return pltpu.make_async_remote_copy(
            source.at[rows(dest, align, count)], target.at[rows(me, align, count)],
            sems.at[0], sems.at[1], device_id={"gz": plane, "pa": dest})

    for other in others:
        send(send_u, recv_u, u_sems, 4, 4, other).start()
    for other in others:
        send(send_a, recv_a, a_sems, 8, 6, other).start()

    def beside(source, target_low, target_high, sems):
        down = pltpu.make_async_remote_copy(
            source, target_high, sems.at[0], sems.at[1], device_id={"gz": plane - 1, "pa": me})
        up = pltpu.make_async_remote_copy(
            source, target_low, sems.at[2], sems.at[3], device_id={"gz": plane + 1, "pa": me})
        return down, up

    def start_beside(pair):
        @pl.when(has_low)
        def _():
            pair[0].start()

        @pl.when(has_high)
        def _():
            pair[1].start()

    def from_beside(pair):
        @pl.when(has_low)
        def _():
            pair[1].wait_recv()

        @pl.when(has_high)
        def _():
            pair[0].wait_recv()

    def left_beside(pair):
        @pl.when(has_low)
        def _():
            pair[0].wait_send()

        @pl.when(has_high)
        def _():
            pair[1].wait_send()

    halo = beside(vel.at[:, 0], low, high, halo_sems)
    uv_halo = beside(uv_send, uv_low, uv_high, uv_sems)
    w_halo = beside(w_send, w_low, w_high, w_sems)

    @pl.when(jnp.logical_not(has_low))
    def _():
        low[...] = jnp.zeros_like(low)
        uv_low[...] = jnp.zeros_like(uv_low)
        w_low[...] = jnp.zeros_like(w_low)

    @pl.when(jnp.logical_not(has_high))
    def _():
        high[...] = jnp.zeros_like(high)
        uv_high[...] = jnp.zeros_like(uv_high)
        w_high[...] = jnp.zeros_like(w_high)

    recv_u[rows(me, 4, 4), :] = send_u[rows(me, 4, 4), :]
    recv_a[rows(me, 8, 6), :] = send_a[rows(me, 8, 6), :]

    def wait_all(ref, sem, count):
        view = ref.at[pl.ds(0, count)]
        pltpu.make_async_copy(view, view, sem).wait()

    for i in rest:
        load(i).wait()
    cos, sin = y_turn[0], y_turn[1]
    def gathered(ref, stride, e):
        return jnp.concatenate([ref[pl.ds(e, 64, stride=stride), :], ref[pl.ds(e + 2, 64, stride=stride), :]], 0)

    def on_grid(blocks):
        turned = y_turned(jnp.concatenate(blocks, 1), cos, sin, y_in)
        return [dot(split(value), y_grid) for value in turned]

    wait_all(recv_u, u_sems.at[1], 4 * (RANKS - 1))
    fields = on_grid([gathered(recv_u, 4, e) for e in range(2)])
    for e in range(2):
        uv_send[e] = fields[e][:, :128]
    start_beside(uv_halo)
    start_beside(halo)
    wait_all(recv_a, a_sems.at[1], 6 * (RANKS - 1))
    row, col = (lax.broadcasted_iota(jnp.int32, (64, 128), i) for i in range(2))
    ky_grid = (TWO_PI / 1024.0) * (8 * row + lax.rem(col, 8)).astype(F32)
    blocks = [gathered(recv_a, 8, e) for e in range(2)]
    curl_re, curl_im = recv_a[pl.ds(4, 64, stride=8), :], recv_a[pl.ds(5, 64, stride=8), :]
    one, two = blocks[0], pltpu.roll(blocks[1], 64, 1)
    pair_one = [jnp.where(left, -(ky_grid * one[64:]), curl_re), jnp.where(left, ky_grid * one[:64], curl_im)]
    pair_two = [jnp.where(left, curl_re, -(ky_grid * two[64:])), jnp.where(left, curl_im, ky_grid * two[:64])]
    fields = fields + on_grid([*blocks, jnp.concatenate(pair_one, 0), jnp.concatenate(pair_two, 0)])
    from_beside(uv_halo)

    def last(parts):
        return dot(y_out, split(jnp.concatenate(parts, 1)))

    sign = jnp.where(lax.broadcasted_iota(jnp.int32, (128, 128), 1) < 64, 0.5, -0.5).astype(F32)
    products = [[], [], []]
    for e in range(2):
        uv, wz, xy = fields[e], fields[2 + e], fields[4 + e]
        uv, vu = uv[:, :128], uv[:, 128:]
        wz, zw = wz[:, :128], wz[:, 128:]
        slope = sign * (uv_high[e] - uv_low[e])
        xy, yx = (xy[:, :128], xy[:, 128:]) if e == 0 else (xy[:, 128:], xy[:, :128])
        xy, yx = xy + pltpu.roll(slope, 64, 1), yx + slope
        products[0].append(vu * zw - wz * yx)
        products[1].append(wz * xy - uv * zw)
        products[2].append(uv * yx)

    def spectral(comp):
        table = y_diff if comp == 2 else y_low
        return last([y_forward(value, cos, sin, table) for value in products[comp]])

    def to_inside(source, target, sems, count):
        for other in others:
            @pl.when(other <= LAST_RANK)
            def _(other=other):
                send(source, target, sems, count, count, other).start()

    modes_w = spectral(2)
    for e in range(2):
        send_w[pl.ds(e, 64, stride=2), :] = modes_w[:, 128 * e : 128 * e + 128]
    to_inside(send_w, recv_w, hz_sems, 2)
    for comp in range(2):
        modes_c = spectral(comp)
        for e in range(2):
            send_c[pl.ds(2 * comp + e, 64, stride=4), :] = modes_c[:, 128 * e : 128 * e + 128]
    to_inside(send_c, recv_c, c_sems, 4)

    inside = me <= LAST_RANK

    from_beside(halo)

    for comp in range(3):
        for i in range(2):
            for a in range(8):
                at = pl.ds(128 * a, 128)
                mid = vel[comp, 0, i, :, at]
                viscous = (high[comp, i, :, at] - 2.0 * mid + low[comp, i, :, at]) - (kx(a) * kx(a) + ky * ky) * mid
                out[comp, 0, i, :, at] = mid + (TIME_STEP * VISCOSITY) * viscous

    plain_cos = [jnp.broadcast_to(x_turn[0, c], (8, 128)) for c in range(8)]
    plain_sin = [jnp.broadcast_to(x_turn[1, c], (8, 128)) for c in range(8)]

    def add_nonlinear(comp, ref, base, stride):
        block = jnp.concatenate([ref[pl.ds(base + e, 64, stride=stride), :] for e in range(2)], 0)
        for a, pair in enumerate(x_forward(block, plain_cos, plain_sin, x_out)):
            at = pl.ds(128 * a, 128)
            keep = mask[:, at].astype(F32) * TIME_STEP
            for i in range(2):
                out[comp, 0, i, :, at] = out[comp, 0, i, :, at] + pair[i] * keep

    @pl.when(inside)
    def _():
        recv_w[rows(me, 2, 2), :] = send_w[rows(me, 2, 2), :]
        recv_c[rows(me, 4, 4), :] = send_c[rows(me, 4, 4), :]
        wait_all(recv_w, hz_sems.at[1], 2 * (RANKS - 1))
        add_nonlinear(2, recv_w, 0, 2)

    w_send[...] = out[2, 0]
    start_beside(w_halo)

    @pl.when(inside)
    def _():
        wait_all(recv_c, c_sems.at[1], 4 * (RANKS - 1))
        add_nonlinear(0, recv_c, 0, 4)
        add_nonlinear(1, recv_c, 2, 4)

    for a in range(8):
        at = pl.ds(128 * a, 128)
        div[0, 0, :, at] = -(kx(a) * out[0, 0, 1, :, at]) - ky * out[1, 0, 1, :, at]
        div[0, 1, :, at] = kx(a) * out[0, 0, 0, :, at] + ky * out[1, 0, 0, :, at]

    from_beside(w_halo)
    div[0] = div[0] + 0.5 * (w_high[...] - w_low[...])

    wait_all(send_u, u_sems.at[0], 4 * (RANKS - 1))
    wait_all(send_a, a_sems.at[0], 6 * (RANKS - 1))

    @pl.when(inside)
    def _():
        wait_all(send_w, hz_sems.at[0], 2 * LAST_RANK)
        wait_all(send_c, c_sems.at[0], 4 * LAST_RANK)

    @pl.when(jnp.logical_not(inside))
    def _():
        wait_all(send_w, hz_sems.at[0], 2 * (LAST_RANK + 1))
        wait_all(send_c, c_sems.at[0], 4 * (LAST_RANK + 1))

    for pair in (halo, uv_halo, w_halo):
        left_beside(pair)


def on_device(velocity, mode_mask):
    constants = tables()
    operands = (velocity, mode_mask, *(jnp.asarray(constants[name]) for name in NAMES))
    whole = pl.BlockSpec(memory_space=pltpu.VMEM)
    dma, vmem = pltpu.SemaphoreType.DMA, pltpu.VMEM
    return pl.pallas_call(
        kernel,
        name="substep",
        out_shape=(
            vmem((3, 1, 2, 8, 1024), F32),
            vmem((1, 2, 8, 1024), F32),
        ),
        in_specs=[pl.BlockSpec(memory_space=pl.ANY)] * len(operands),
        out_specs=(whole, whole),
        scratch_shapes=[
            *(vmem(operand.shape, operand.dtype) for operand in operands), dma((len(operands),)),
            vmem((256, 128), F32), vmem((256, 128), F32),
            vmem((512, 128), F32), vmem((512, 128), F32),
            vmem((128, 128), F32), vmem((128, 128), F32),
            vmem((256, 128), F32), vmem((256, 128), F32),
            *[vmem((2, 128, 128), F32)] * 3,
            *[vmem((3, 2, 8, 1024), F32)] * 2,
            *[vmem((2, 8, 1024), F32)] * 3,
            *[dma((2,))] * 4, *[dma((4,))] * 3,
        ],
        compiler_params=pltpu.CompilerParams(collective_id=0, has_side_effects=True),
    )(*operands)


def solution(mesh):
    return jax.shard_map(
        on_device,
        mesh=mesh,
        in_specs=(P(None, "gz", None, "pa", None), P("pa", None)),
        out_specs=(P(None, "gz", None, "pa", None), P("gz", None, "pa", None)),
        check_vma=False,
    )
```

```python
import math

import jax
import jax.numpy as jnp
import numpy as np
from jax import lax
from jax.experimental import pallas as pl
from jax.experimental.pallas import tpu as pltpu
from jax.sharding import PartitionSpec as P


TWO_PI = 2.0 * math.pi
TIME_STEP = 0.2
VISCOSITY = 0.25
RANKS = 64
LAST_RANK = 42
F32 = jnp.float32
BF16 = jnp.bfloat16


def halves(table):
    table = np.asarray(table, np.float32)
    high = table.astype(jnp.bfloat16)
    low = (table - high.astype(np.float32)).astype(jnp.bfloat16)
    return np.stack([high, low])


def tables():
    index = np.arange
    p, b, c, s, q, r = index(64), index(128), index(8), index(8), index(64), index(128)
    d = (2 * p[None, :] + index(2)[:, None]).reshape(-1)
    angle = TWO_PI / 128.0 * (d[:, None] * b[None, :] % 128)
    cos, sin = np.cos(angle) / 32.0, np.sin(angle) / 32.0
    x_in = np.block([[cos, -sin], [sin, cos]])
    angle = TWO_PI / 1024.0 * (c[:, None] * b[None, :])
    x_turn = np.stack([np.cos(angle), np.sin(angle)]).astype(np.float32).reshape(2, 8, 1, 128)
    angle = TWO_PI / 128.0 * (r[:, None] * q[None, :] % 128)
    cos, sin = np.cos(angle) / 32.0, np.sin(angle) / 32.0
    y_in = np.block([[cos, -sin], [sin, cos]])
    angle = TWO_PI / 1024.0 * (r[:, None] * np.tile(s, 16)[None, :])
    y_turn = np.stack([np.cos(angle), np.sin(angle)]).astype(np.float32)
    angle = TWO_PI / 8.0 * (s[:, None] * s[None, :] % 8)
    cos8, sin8 = np.cos(angle), np.sin(angle)
    eye = np.eye(8)
    real = np.kron(np.eye(2), np.kron(eye, cos8))
    imag = np.kron(np.eye(2), np.kron(eye, -sin8))
    both = np.concatenate([real, imag], 0)
    y_grid = np.concatenate([both, np.roll(both, 64, axis=1)], 1)
    real = np.kron(eye, cos8) / 32.0
    imag = np.kron(eye, -sin8) / 32.0
    line = np.concatenate([real, imag, imag, -real], 1)
    y_low = np.concatenate([line, np.zeros_like(line)], 0)
    y_diff = np.concatenate([line, -line], 0)
    angle = TWO_PI / 128.0 * (q[:, None] * r[None, :] % 128)
    y_out = np.concatenate([np.cos(angle), np.sin(angle)], 1)
    angle = TWO_PI / 128.0 * (d[:, None] * b[None, :] % 128)
    x_out = np.concatenate([np.cos(angle), np.sin(angle)], 1) / 32.0
    return dict(
        x_in=halves(x_in),
        x_turn=x_turn,
        y_in=halves(y_in),
        y_turn=y_turn,
        y_grid=halves(y_grid),
        y_low=halves(y_low),
        y_diff=halves(y_diff),
        y_out=halves(y_out),
        x_out=halves(x_out),
    )


NAMES = ("x_in", "x_turn", "y_in", "y_turn", "y_grid", "y_low", "y_diff", "y_out", "x_out")


def split(value):
    high = value.astype(BF16)
    return high, (value - high.astype(F32)).astype(BF16)


def dot(left, right, contract=((1,), (0,))):
    def one(i, j):
        return lax.dot_general(left[i], right[j], (contract, ((), ())), preferred_element_type=F32)

    return one(0, 0) + (one(0, 1) + one(1, 0))


def eight(values, sign):
    count = len(values)
    if count == 1:
        return values
    even, odd = eight(values[0::2], sign), eight(values[1::2], sign)
    half = count // 2
    low, high = [], []
    for k in range(half):
        (er, ei), (qr, qi) = even[k], odd[k]
        turn = 8 // count * k
        if turn == 0:
            tr, ti = qr, qi
        elif turn == 2:
            tr, ti = -sign * qi, sign * qr
        else:
            root = math.sqrt(0.5)
            if turn == 1:
                tr, ti = root * (qr - sign * qi), root * (qi + sign * qr)
            else:
                tr, ti = -root * (qr + sign * qi), root * (sign * qr - qi)
        low.append((er + tr, ei + ti))
        high.append((er - tr, ei - ti))
    return low + high


def x_inverse(fields, turn_cos, turn_sin, table):
    real, imag = [], []
    for field in fields:
        for c, (vr, vi) in enumerate(eight(field, 1.0)):
            real.append(vr * turn_cos[c] - vi * turn_sin[c])
            imag.append(vr * turn_sin[c] + vi * turn_cos[c])
    lines = jnp.concatenate([jnp.concatenate(real, 0), jnp.concatenate(imag, 0)], 1)
    return dot(table, split(lines), ((1,), (1,)))


def y_turned(modes, cos, sin, table):
    lines = dot(table, split(modes))
    out = []
    for k in range(modes.shape[1] // 128):
        vr, vi = lines[:128, 128 * k : 128 * k + 128], lines[128:, 128 * k : 128 * k + 128]
        out.append(jnp.concatenate([vr * cos - vi * sin, vr * sin + vi * cos], 1))
    return out


def y_forward(product, cos, sin, table):
    line = dot(split(product), table)
    one, two = line[:, :128], line[:, 128:]
    return jnp.concatenate([one * cos + two * sin, two * cos - one * sin], 0)


def x_forward(block, turn_cos, turn_sin, table):
    line = dot(split(block.T), table)
    values = []
    for c in range(8):
        re, im = line[8 * c : 8 * c + 8], line[64 + 8 * c : 72 + 8 * c]
        vr, vi = re[:, :128] + im[:, 128:], im[:, :128] - re[:, 128:]
        values.append((vr * turn_cos[c] + vi * turn_sin[c], vi * turn_cos[c] - vr * turn_sin[c]))
    return eight(values, -1.0)


HOPS = [(dy, dz, dx) for dz in (1, 0) for dy in (4, 5, 3, 6, 2, 7, 1, 0) for dx in (2, 3, 1, 0)][:-1]


def hops(hop):
    dy, dz, dx = hop
    return min(dy, 8 - dy) + 4 * dz + min(dx, 4 - dx)


FAR = sorted(range(63), key=lambda i: -hops(HOPS[i]))


def partners(me):
    x, z, y = lax.rem(me, 4), lax.rem(lax.div(me, 4), 2), lax.div(me, 8)
    xs = [lax.rem(x + i, 4) for i in range(4)]
    zs = [4 * lax.rem(z + i, 2) for i in range(2)]
    ys = [8 * lax.rem(y + i, 8) for i in range(8)]
    return [ys[dy] + zs[dz] + xs[dx] for dy, dz, dx in HOPS]


def rows(start, align, count):
    return pl.ds(pl.multiple_of(start * align, align), count)


def kernel(*refs):
    count = 2 + len(NAMES)
    sources, out, div, held = refs[:count], refs[count], refs[count + 1], refs[count + 2 : 2 * count + 2]
    body(sources, held, out, div, *refs[2 * count + 2 :])


def body(sources, held, out, div, load_sems,
           send_u, recv_u, send_a, recv_a, send_w, recv_w, send_c, recv_c, uv_send, uv_low, uv_high,
           low, high, w_low, w_high, w_send, u_sems, a_sems, hz_sems, c_sems, uv_sems, halo_sems, w_sems):
    me, plane = lax.axis_index("pa"), lax.axis_index("gz")
    barrier = pltpu.get_barrier_semaphore()
    vel, mask, x_in, x_turn, y_in, y_turn, y_grid, y_low, y_diff, y_out, x_out = held

    def load(i):
        return pltpu.make_async_copy(sources[i], held[i], load_sems.at[i])

    others = partners(me)
    for other in (others[i] for i in FAR):
        pl.semaphore_signal(barrier, inc=1, device_id={"gz": plane, "pa": other})
    has_low, has_high = plane > 0, plane < 7

    @pl.when(has_low)
    def _():
        pl.semaphore_signal(barrier, inc=1, device_id={"gz": plane - 1, "pa": me})

    @pl.when(has_high)
    def _():
        pl.semaphore_signal(barrier, inc=1, device_id={"gz": plane + 1, "pa": me})

    rest = [i for i in range(len(held)) if i not in (0, 2, 3)]
    for i in (0, 2, 3, *rest):
        load(i).start()
    sub = lax.broadcasted_iota(jnp.int32, (8, 128), 0)
    lane = lax.broadcasted_iota(jnp.int32, (8, 128), 1)
    modes = me * 8 + sub
    ky = (TWO_PI / 1024.0) * modes.astype(F32)
    weight = jnp.where(modes == 0, 1.0, 2.0).astype(F32)

    def kx(a):
        return (TWO_PI / 1024.0) * (lane + (128 * a - 1024 * (a // 4))).astype(F32)

    def piece(ref, *lead):
        return [ref[(*lead, slice(None), pl.ds(128 * a, 128))] for a in range(8)]

    for i in (0, 2, 3):
        load(i).wait()
    turn_cos = [weight * x_turn[0, c] for c in range(8)]
    turn_sin = [weight * x_turn[1, c] for c in range(8)]

    def field(comp):
        return list(zip(piece(vel, comp, 0, 0), piece(vel, comp, 0, 1), strict=True))

    u, v, w = field(0), field(1), field(2)
    omega_z = [
        (ky * u[a][1] - kx(a) * v[a][1], kx(a) * v[a][0] - ky * u[a][0]) for a in range(8)
    ]
    curl_y = [(kx(a) * w[a][1], -(kx(a) * w[a][0])) for a in range(8)]
    grid = x_inverse([u, v, w, omega_z, curl_y, curl_y], turn_cos, turn_sin, x_in)
    left = lax.broadcasted_iota(jnp.int32, (64, 128), 1) < 64
    for j in range(4):
        send_u[pl.ds(j, 64, stride=4), :] = grid[64 * j : 64 * j + 64, :128]
        send_a[pl.ds(j, 64, stride=8), :] = grid[64 * j : 64 * j + 64, 128:256]
    for ri in range(2):
        first, second = (grid[128 * ri + 64 * e : 128 * ri + 64 * e + 64, 256:] for e in range(2))
        send_a[pl.ds(4 + ri, 64, stride=8), :] = jnp.where(left, second, first)

    @pl.when(jnp.logical_and(has_low, has_high))
    def _():
        pl.semaphore_wait(barrier, RANKS + 1)

    @pl.when(jnp.logical_not(jnp.logical_and(has_low, has_high)))
    def _():
        pl.semaphore_wait(barrier, RANKS)

    def send(source, target, sems, align, count, dest):
        return pltpu.make_async_remote_copy(
            source.at[rows(dest, align, count)], target.at[rows(me, align, count)],
            sems.at[0], sems.at[1], device_id={"gz": plane, "pa": dest})

    for other in others:
        send(send_u, recv_u, u_sems, 4, 4, other).start()
    for other in others:
        send(send_a, recv_a, a_sems, 8, 6, other).start()

    def beside(source, target_low, target_high, sems):
        down = pltpu.make_async_remote_copy(
            source, target_high, sems.at[0], sems.at[1], device_id={"gz": plane - 1, "pa": me})
        up = pltpu.make_async_remote_copy(
            source, target_low, sems.at[2], sems.at[3], device_id={"gz": plane + 1, "pa": me})
        return down, up

    def start_beside(pair):
        @pl.when(has_low)
        def _():
            pair[0].start()

        @pl.when(has_high)
        def _():
            pair[1].start()

    def from_beside(pair):
        @pl.when(has_low)
        def _():
            pair[1].wait_recv()

        @pl.when(has_high)
        def _():
            pair[0].wait_recv()

    def left_beside(pair):
        @pl.when(has_low)
        def _():
            pair[0].wait_send()

        @pl.when(has_high)
        def _():
            pair[1].wait_send()

    halo = beside(vel.at[:, 0], low, high, halo_sems)
    uv_halo = beside(uv_send, uv_low, uv_high, uv_sems)
    w_halo = beside(w_send, w_low, w_high, w_sems)

    @pl.when(jnp.logical_not(has_low))
    def _():
        low[...] = jnp.zeros_like(low)
        uv_low[...] = jnp.zeros_like(uv_low)
        w_low[...] = jnp.zeros_like(w_low)

    @pl.when(jnp.logical_not(has_high))
    def _():
        high[...] = jnp.zeros_like(high)
        uv_high[...] = jnp.zeros_like(uv_high)
        w_high[...] = jnp.zeros_like(w_high)

    recv_u[rows(me, 4, 4), :] = send_u[rows(me, 4, 4), :]
    recv_a[rows(me, 8, 6), :] = send_a[rows(me, 8, 6), :]

    def wait_all(ref, sem, count):
        view = ref.at[pl.ds(0, count)]
        pltpu.make_async_copy(view, view, sem).wait()

    for i in rest:
        load(i).wait()
    cos, sin = y_turn[0], y_turn[1]
    def gathered(ref, stride, e):
        return jnp.concatenate([ref[pl.ds(e, 64, stride=stride), :], ref[pl.ds(e + 2, 64, stride=stride), :]], 0)

    def on_grid(blocks):
        turned = y_turned(jnp.concatenate(blocks, 1), cos, sin, y_in)
        return [dot(split(value), y_grid) for value in turned]

    wait_all(recv_u, u_sems.at[1], 4 * (RANKS - 1))
    fields = on_grid([gathered(recv_u, 4, e) for e in range(2)])
    for e in range(2):
        uv_send[e] = fields[e][:, :128]
    start_beside(uv_halo)
    wait_all(recv_a, a_sems.at[1], 6 * (RANKS - 1))
    start_beside(halo)
    row, col = (lax.broadcasted_iota(jnp.int32, (64, 128), i) for i in range(2))
    ky_grid = (TWO_PI / 1024.0) * (8 * row + lax.rem(col, 8)).astype(F32)
    blocks = [gathered(recv_a, 8, e) for e in range(2)]
    curl_re, curl_im = recv_a[pl.ds(4, 64, stride=8), :], recv_a[pl.ds(5, 64, stride=8), :]
    one, two = blocks[0], pltpu.roll(blocks[1], 64, 1)
    pair_one = [jnp.where(left, -(ky_grid * one[64:]), curl_re), jnp.where(left, ky_grid * one[:64], curl_im)]
    pair_two = [jnp.where(left, curl_re, -(ky_grid * two[64:])), jnp.where(left, curl_im, ky_grid * two[:64])]
    fields = fields + on_grid([*blocks, jnp.concatenate(pair_one, 0), jnp.concatenate(pair_two, 0)])
    from_beside(uv_halo)

    def last(parts):
        return dot(y_out, split(jnp.concatenate(parts, 1)))

    sign = jnp.where(lax.broadcasted_iota(jnp.int32, (128, 128), 1) < 64, 0.5, -0.5).astype(F32)
    products = [[], [], []]
    for e in range(2):
        uv, wz, xy = fields[e], fields[2 + e], fields[4 + e]
        uv, vu = uv[:, :128], uv[:, 128:]
        wz, zw = wz[:, :128], wz[:, 128:]
        slope = sign * (uv_high[e] - uv_low[e])
        xy, yx = (xy[:, :128], xy[:, 128:]) if e == 0 else (xy[:, 128:], xy[:, :128])
        xy, yx = xy + pltpu.roll(slope, 64, 1), yx + slope
        products[0].append(vu * zw - wz * yx)
        products[1].append(wz * xy - uv * zw)
        products[2].append(uv * yx)

    def spectral(comp):
        table = y_diff if comp == 2 else y_low
        return last([y_forward(value, cos, sin, table) for value in products[comp]])

    def to_inside(source, target, sems, count):
        for other in (others[i] for i in FAR):
            @pl.when(other <= LAST_RANK)
            def _(other=other):
                send(source, target, sems, count, count, other).start()

    modes_w = spectral(2)
    for e in range(2):
        send_w[pl.ds(e, 64, stride=2), :] = modes_w[:, 128 * e : 128 * e + 128]
    to_inside(send_w, recv_w, hz_sems, 2)
    for comp in range(2):
        modes_c = spectral(comp)
        for e in range(2):
            send_c[pl.ds(2 * comp + e, 64, stride=4), :] = modes_c[:, 128 * e : 128 * e + 128]
    to_inside(send_c, recv_c, c_sems, 4)

    inside = me <= LAST_RANK

    from_beside(halo)

    for comp in range(3):
        for i in range(2):
            for a in range(8):
                at = pl.ds(128 * a, 128)
                mid = vel[comp, 0, i, :, at]
                viscous = (high[comp, i, :, at] - 2.0 * mid + low[comp, i, :, at]) - (kx(a) * kx(a) + ky * ky) * mid
                out[comp, 0, i, :, at] = mid + (TIME_STEP * VISCOSITY) * viscous

    plain_cos = [jnp.broadcast_to(x_turn[0, c], (8, 128)) for c in range(8)]
    plain_sin = [jnp.broadcast_to(x_turn[1, c], (8, 128)) for c in range(8)]

    def add_nonlinear(comp, ref, base, stride):
        block = jnp.concatenate([ref[pl.ds(base + e, 64, stride=stride), :] for e in range(2)], 0)
        for a, pair in enumerate(x_forward(block, plain_cos, plain_sin, x_out)):
            at = pl.ds(128 * a, 128)
            keep = mask[:, at].astype(F32) * TIME_STEP
            for i in range(2):
                out[comp, 0, i, :, at] = out[comp, 0, i, :, at] + pair[i] * keep

    @pl.when(inside)
    def _():
        recv_w[rows(me, 2, 2), :] = send_w[rows(me, 2, 2), :]
        recv_c[rows(me, 4, 4), :] = send_c[rows(me, 4, 4), :]
        wait_all(recv_w, hz_sems.at[1], 2 * (RANKS - 1))
        add_nonlinear(2, recv_w, 0, 2)

    w_send[...] = out[2, 0]
    start_beside(w_halo)

    @pl.when(inside)
    def _():
        wait_all(recv_c, c_sems.at[1], 4 * (RANKS - 1))
        add_nonlinear(0, recv_c, 0, 4)
        add_nonlinear(1, recv_c, 2, 4)

    for a in range(8):
        at = pl.ds(128 * a, 128)
        div[0, 0, :, at] = -(kx(a) * out[0, 0, 1, :, at]) - ky * out[1, 0, 1, :, at]
        div[0, 1, :, at] = kx(a) * out[0, 0, 0, :, at] + ky * out[1, 0, 0, :, at]

    from_beside(w_halo)
    div[0] = div[0] + 0.5 * (w_high[...] - w_low[...])

    wait_all(send_u, u_sems.at[0], 4 * (RANKS - 1))
    wait_all(send_a, a_sems.at[0], 6 * (RANKS - 1))

    @pl.when(inside)
    def _():
        wait_all(send_w, hz_sems.at[0], 2 * LAST_RANK)
        wait_all(send_c, c_sems.at[0], 4 * LAST_RANK)

    @pl.when(jnp.logical_not(inside))
    def _():
        wait_all(send_w, hz_sems.at[0], 2 * (LAST_RANK + 1))
        wait_all(send_c, c_sems.at[0], 4 * (LAST_RANK + 1))

    for pair in (halo, uv_halo, w_halo):
        left_beside(pair)


def store(following, divergence, out, div, sems):
    copies = [
        pltpu.make_async_copy(following, out, sems.at[0]),
        pltpu.make_async_copy(divergence, div, sems.at[1]),
    ]
    for copy in copies:
        copy.start()
    for copy in copies:
        copy.wait()


def on_device(velocity, mode_mask):
    constants = tables()
    operands = (velocity, mode_mask, *(jnp.asarray(constants[name]) for name in NAMES))
    whole = pl.BlockSpec(memory_space=pltpu.VMEM)
    dma, vmem = pltpu.SemaphoreType.DMA, pltpu.VMEM
    held = pl.pallas_call(
        kernel,
        name="substep",
        out_shape=(
            vmem((3, 1, 2, 8, 1024), F32),
            vmem((1, 2, 8, 1024), F32),
        ),
        in_specs=[pl.BlockSpec(memory_space=pl.ANY)] * len(operands),
        out_specs=(whole, whole),
        scratch_shapes=[
            *(vmem(operand.shape, operand.dtype) for operand in operands), dma((len(operands),)),
            vmem((256, 128), F32), vmem((256, 128), F32),
            vmem((512, 128), F32), vmem((512, 128), F32),
            vmem((128, 128), F32), vmem((128, 128), F32),
            vmem((256, 128), F32), vmem((256, 128), F32),
            *[vmem((2, 128, 128), F32)] * 3,
            *[vmem((3, 2, 8, 1024), F32)] * 2,
            *[vmem((2, 8, 1024), F32)] * 3,
            *[dma((2,))] * 4, *[dma((4,))] * 3,
        ],
        compiler_params=pltpu.CompilerParams(collective_id=0, has_side_effects=True),
    )(*operands)
    return pl.pallas_call(
        store,
        name="store",
        out_shape=(
            jax.ShapeDtypeStruct((3, 1, 2, 8, 1024), F32),
            jax.ShapeDtypeStruct((1, 2, 8, 1024), F32),
        ),
        in_specs=[whole, whole],
        out_specs=[pl.BlockSpec(memory_space=pl.ANY)] * 2,
        scratch_shapes=[dma((2,))],
    )(*(pltpu.with_memory_space_constraint(value, pltpu.VMEM) for value in held))


def solution(mesh):
    return jax.shard_map(
        on_device,
        mesh=mesh,
        in_specs=(P(None, "gz", None, "pa", None), P("pa", None)),
        out_specs=(P(None, "gz", None, "pa", None), P("gz", None, "pa", None)),
        check_vma=False,
    )
```

```python
import math

import jax
import jax.numpy as jnp
import numpy as np
from jax import lax
from jax.experimental import pallas as pl
from jax.experimental.pallas import tpu as pltpu
from jax.sharding import PartitionSpec as P


TWO_PI = 2.0 * math.pi
TIME_STEP = 0.2
VISCOSITY = 0.25
RANKS = 64
LAST_RANK = 42
F32 = jnp.float32
BF16 = jnp.bfloat16


def halves(table):
    table = np.asarray(table, np.float32)
    high = table.astype(jnp.bfloat16)
    low = (table - high.astype(np.float32)).astype(jnp.bfloat16)
    return np.stack([high, low])


def tables():
    index = np.arange
    p, b, c, s, q, r = index(64), index(128), index(8), index(8), index(64), index(128)
    d = (2 * p[None, :] + index(2)[:, None]).reshape(-1)
    angle = TWO_PI / 128.0 * (d[:, None] * b[None, :] % 128)
    cos, sin = np.cos(angle) / 32.0, np.sin(angle) / 32.0
    x_in = np.block([[cos, -sin], [sin, cos]])
    angle = TWO_PI / 1024.0 * (c[:, None] * b[None, :])
    x_turn = np.stack([np.cos(angle), np.sin(angle)]).astype(np.float32).reshape(2, 8, 1, 128)
    angle = TWO_PI / 128.0 * (r[:, None] * q[None, :] % 128)
    cos, sin = np.cos(angle) / 32.0, np.sin(angle) / 32.0
    y_in = np.block([[cos, -sin], [sin, cos]])
    angle = TWO_PI / 1024.0 * (r[:, None] * np.tile(s, 16)[None, :])
    y_turn = np.stack([np.cos(angle), np.sin(angle)]).astype(np.float32)
    angle = TWO_PI / 8.0 * (s[:, None] * s[None, :] % 8)
    cos8, sin8 = np.cos(angle), np.sin(angle)
    eye = np.eye(8)
    real = np.kron(np.eye(2), np.kron(eye, cos8))
    imag = np.kron(np.eye(2), np.kron(eye, -sin8))
    both = np.concatenate([real, imag], 0)
    y_grid = np.concatenate([both, np.roll(both, 64, axis=1)], 1)
    real = np.kron(eye, cos8) / 32.0
    imag = np.kron(eye, -sin8) / 32.0
    line = np.concatenate([real, imag, imag, -real], 1)
    y_low = np.concatenate([line, np.zeros_like(line)], 0)
    y_diff = np.concatenate([line, -line], 0)
    angle = TWO_PI / 128.0 * (q[:, None] * r[None, :] % 128)
    y_out = np.concatenate([np.cos(angle), np.sin(angle)], 1)
    angle = TWO_PI / 128.0 * (d[:, None] * b[None, :] % 128)
    x_out = np.concatenate([np.cos(angle), np.sin(angle)], 1) / 32.0
    return dict(
        x_in=halves(x_in),
        x_turn=x_turn,
        y_in=halves(y_in),
        y_turn=y_turn,
        y_grid=halves(y_grid),
        y_low=halves(y_low),
        y_diff=halves(y_diff),
        y_out=halves(y_out),
        x_out=halves(x_out),
    )


NAMES = ("x_in", "x_turn", "y_in", "y_turn", "y_grid", "y_low", "y_diff", "y_out", "x_out")


def split(value):
    high = value.astype(BF16)
    return high, (value - high.astype(F32)).astype(BF16)


def dot(left, right, contract=((1,), (0,))):
    def one(i, j):
        return lax.dot_general(left[i], right[j], (contract, ((), ())), preferred_element_type=F32)

    return one(0, 0) + (one(0, 1) + one(1, 0))


def eight(values, sign):
    count = len(values)
    if count == 1:
        return values
    even, odd = eight(values[0::2], sign), eight(values[1::2], sign)
    half = count // 2
    low, high = [], []
    for k in range(half):
        (er, ei), (qr, qi) = even[k], odd[k]
        turn = 8 // count * k
        if turn == 0:
            tr, ti = qr, qi
        elif turn == 2:
            tr, ti = -sign * qi, sign * qr
        else:
            root = math.sqrt(0.5)
            if turn == 1:
                tr, ti = root * (qr - sign * qi), root * (qi + sign * qr)
            else:
                tr, ti = -root * (qr + sign * qi), root * (sign * qr - qi)
        low.append((er + tr, ei + ti))
        high.append((er - tr, ei - ti))
    return low + high


def x_inverse(fields, turn_cos, turn_sin, table):
    real, imag = [], []
    for field in fields:
        for c, (vr, vi) in enumerate(eight(field, 1.0)):
            real.append(vr * turn_cos[c] - vi * turn_sin[c])
            imag.append(vr * turn_sin[c] + vi * turn_cos[c])
    lines = jnp.concatenate([jnp.concatenate(real, 0), jnp.concatenate(imag, 0)], 1)
    return dot(table, split(lines), ((1,), (1,)))


def y_turned(modes, cos, sin, table):
    lines = dot(table, split(modes))
    out = []
    for k in range(modes.shape[1] // 128):
        vr, vi = lines[:128, 128 * k : 128 * k + 128], lines[128:, 128 * k : 128 * k + 128]
        out.append(jnp.concatenate([vr * cos - vi * sin, vr * sin + vi * cos], 1))
    return out


def y_forward(product, cos, sin, table):
    line = dot(split(product), table)
    one, two = line[:, :128], line[:, 128:]
    return jnp.concatenate([one * cos + two * sin, two * cos - one * sin], 0)


def x_forward(block, turn_cos, turn_sin, table):
    line = dot(split(block.T), table)
    values = []
    for c in range(8):
        re, im = line[8 * c : 8 * c + 8], line[64 + 8 * c : 72 + 8 * c]
        vr, vi = re[:, :128] + im[:, 128:], im[:, :128] - re[:, 128:]
        values.append((vr * turn_cos[c] + vi * turn_sin[c], vi * turn_cos[c] - vr * turn_sin[c]))
    return eight(values, -1.0)


HOPS = [(dy, dz, dx) for dz in (1, 0) for dy in (4, 5, 3, 6, 2, 7, 1, 0) for dx in (2, 3, 1, 0)][:-1]


def hops(hop):
    dy, dz, dx = hop
    return min(dy, 8 - dy) + 4 * dz + min(dx, 4 - dx)


FAR = sorted(range(63), key=lambda i: -hops(HOPS[i]))


def partners(me):
    x, z, y = lax.rem(me, 4), lax.rem(lax.div(me, 4), 2), lax.div(me, 8)
    xs = [lax.rem(x + i, 4) for i in range(4)]
    zs = [4 * lax.rem(z + i, 2) for i in range(2)]
    ys = [8 * lax.rem(y + i, 8) for i in range(8)]
    return [ys[dy] + zs[dz] + xs[dx] for dy, dz, dx in HOPS]


def rows(start, align, count):
    return pl.ds(pl.multiple_of(start * align, align), count)


def kernel(*refs):
    count = 2 + len(NAMES)
    sources, out, div, held = refs[:count], refs[count], refs[count + 1], refs[count + 2 : 2 * count + 2]
    body(sources, held, out, div, *refs[2 * count + 2 :])


def body(sources, held, out, div, load_sems,
           send_u, recv_u, send_a, recv_a, send_w, recv_w, send_c, recv_c, uv_send, uv_low, uv_high,
           low, high, w_low, w_high, w_send, u_sems, a_sems, hz_sems, c_sems, uv_sems, halo_sems, w_sems):
    me, plane = lax.axis_index("pa"), lax.axis_index("gz")
    barrier = pltpu.get_barrier_semaphore()
    vel, mask, x_in, x_turn, y_in, y_turn, y_grid, y_low, y_diff, y_out, x_out = held

    def load(i):
        return pltpu.make_async_copy(sources[i], held[i], load_sems.at[i])

    others = partners(me)
    for other in (others[i] for i in FAR):
        pl.semaphore_signal(barrier, inc=1, device_id={"gz": plane, "pa": other})
    has_low, has_high = plane > 0, plane < 7

    @pl.when(has_low)
    def _():
        pl.semaphore_signal(barrier, inc=1, device_id={"gz": plane - 1, "pa": me})

    @pl.when(has_high)
    def _():
        pl.semaphore_signal(barrier, inc=1, device_id={"gz": plane + 1, "pa": me})

    rest = [i for i in range(len(held)) if i not in (0, 2, 3)]
    for i in (0, 2, 3, *rest):
        load(i).start()
    sub = lax.broadcasted_iota(jnp.int32, (8, 128), 0)
    lane = lax.broadcasted_iota(jnp.int32, (8, 128), 1)
    modes = me * 8 + sub
    ky = (TWO_PI / 1024.0) * modes.astype(F32)
    weight = jnp.where(modes == 0, 1.0, 2.0).astype(F32)

    def kx(a):
        return (TWO_PI / 1024.0) * (lane + (128 * a - 1024 * (a // 4))).astype(F32)

    def piece(ref, *lead):
        return [ref[(*lead, slice(None), pl.ds(128 * a, 128))] for a in range(8)]

    for i in (0, 2, 3):
        load(i).wait()
    turn_cos = [weight * x_turn[0, c] for c in range(8)]
    turn_sin = [weight * x_turn[1, c] for c in range(8)]

    def field(comp):
        return list(zip(piece(vel, comp, 0, 0), piece(vel, comp, 0, 1), strict=True))

    u, v, w = field(0), field(1), field(2)
    omega_z = [
        (ky * u[a][1] - kx(a) * v[a][1], kx(a) * v[a][0] - ky * u[a][0]) for a in range(8)
    ]
    curl_y = [(kx(a) * w[a][1], -(kx(a) * w[a][0])) for a in range(8)]
    grid = x_inverse([u, v, w, omega_z, curl_y, curl_y], turn_cos, turn_sin, x_in)
    left = lax.broadcasted_iota(jnp.int32, (64, 128), 1) < 64
    for j in range(4):
        send_u[pl.ds(j, 64, stride=4), :] = grid[64 * j : 64 * j + 64, :128]
        send_a[pl.ds(j, 64, stride=8), :] = grid[64 * j : 64 * j + 64, 128:256]
    for ri in range(2):
        first, second = (grid[128 * ri + 64 * e : 128 * ri + 64 * e + 64, 256:] for e in range(2))
        send_a[pl.ds(4 + ri, 64, stride=8), :] = jnp.where(left, second, first)

    @pl.when(jnp.logical_and(has_low, has_high))
    def _():
        pl.semaphore_wait(barrier, RANKS + 1)

    @pl.when(jnp.logical_not(jnp.logical_and(has_low, has_high)))
    def _():
        pl.semaphore_wait(barrier, RANKS)

    def send(source, target, sems, align, count, dest):
        return pltpu.make_async_remote_copy(
            source.at[rows(dest, align, count)], target.at[rows(me, align, count)],
            sems.at[0], sems.at[1], device_id={"gz": plane, "pa": dest})

    for other in others:
        send(send_u, recv_u, u_sems, 4, 4, other).start()
    for other in others:
        send(send_a, recv_a, a_sems, 8, 6, other).start()

    def beside(source, target_low, target_high, sems):
        down = pltpu.make_async_remote_copy(
            source, target_high, sems.at[0], sems.at[1], device_id={"gz": plane - 1, "pa": me})
        up = pltpu.make_async_remote_copy(
            source, target_low, sems.at[2], sems.at[3], device_id={"gz": plane + 1, "pa": me})
        return down, up

    def start_beside(pair):
        @pl.when(has_low)
        def _():
            pair[0].start()

        @pl.when(has_high)
        def _():
            pair[1].start()

    def from_beside(pair):
        @pl.when(has_low)
        def _():
            pair[1].wait_recv()

        @pl.when(has_high)
        def _():
            pair[0].wait_recv()

    def left_beside(pair):
        @pl.when(has_low)
        def _():
            pair[0].wait_send()

        @pl.when(has_high)
        def _():
            pair[1].wait_send()

    halo = beside(vel.at[:, 0], low, high, halo_sems)
    uv_halo = [beside(uv_send.at[e], uv_low.at[e], uv_high.at[e], uv_sems.at[e]) for e in range(2)]
    w_halo = beside(w_send, w_low, w_high, w_sems)

    @pl.when(jnp.logical_not(has_low))
    def _():
        low[...] = jnp.zeros_like(low)
        uv_low[...] = jnp.zeros_like(uv_low)
        w_low[...] = jnp.zeros_like(w_low)

    @pl.when(jnp.logical_not(has_high))
    def _():
        high[...] = jnp.zeros_like(high)
        uv_high[...] = jnp.zeros_like(uv_high)
        w_high[...] = jnp.zeros_like(w_high)

    recv_u[rows(me, 4, 4), :] = send_u[rows(me, 4, 4), :]
    recv_a[rows(me, 8, 6), :] = send_a[rows(me, 8, 6), :]

    def wait_all(ref, sem, count):
        view = ref.at[pl.ds(0, count)]
        pltpu.make_async_copy(view, view, sem).wait()

    for i in rest:
        load(i).wait()
    cos, sin = y_turn[0], y_turn[1]
    def gathered(ref, stride, e):
        return jnp.concatenate([ref[pl.ds(e, 64, stride=stride), :], ref[pl.ds(e + 2, 64, stride=stride), :]], 0)

    def on_grid(blocks):
        turned = y_turned(jnp.concatenate(blocks, 1), cos, sin, y_in)
        return [dot(split(value), y_grid) for value in turned]

    wait_all(recv_u, u_sems.at[1], 4 * (RANKS - 1))
    fields = []
    for e in range(2):
        fields += on_grid([gathered(recv_u, 4, e)])
        uv_send[e] = fields[e][:, :128]
        start_beside(uv_halo[e])
    wait_all(recv_a, a_sems.at[1], 6 * (RANKS - 1))
    start_beside(halo)
    row, col = (lax.broadcasted_iota(jnp.int32, (64, 128), i) for i in range(2))
    ky_grid = (TWO_PI / 1024.0) * (8 * row + lax.rem(col, 8)).astype(F32)
    blocks = [gathered(recv_a, 8, e) for e in range(2)]
    curl_re, curl_im = recv_a[pl.ds(4, 64, stride=8), :], recv_a[pl.ds(5, 64, stride=8), :]
    one, two = blocks[0], pltpu.roll(blocks[1], 64, 1)
    pair_one = [jnp.where(left, -(ky_grid * one[64:]), curl_re), jnp.where(left, ky_grid * one[:64], curl_im)]
    pair_two = [jnp.where(left, curl_re, -(ky_grid * two[64:])), jnp.where(left, curl_im, ky_grid * two[:64])]
    fields = fields + on_grid([*blocks, jnp.concatenate(pair_one, 0), jnp.concatenate(pair_two, 0)])
    for pair in uv_halo:
        from_beside(pair)

    def last(parts):
        return dot(y_out, split(jnp.concatenate(parts, 1)))

    sign = jnp.where(lax.broadcasted_iota(jnp.int32, (128, 128), 1) < 64, 0.5, -0.5).astype(F32)
    products = [[], [], []]
    for e in range(2):
        uv, wz, xy = fields[e], fields[2 + e], fields[4 + e]
        uv, vu = uv[:, :128], uv[:, 128:]
        wz, zw = wz[:, :128], wz[:, 128:]
        slope = sign * (uv_high[e] - uv_low[e])
        xy, yx = (xy[:, :128], xy[:, 128:]) if e == 0 else (xy[:, 128:], xy[:, :128])
        xy, yx = xy + pltpu.roll(slope, 64, 1), yx + slope
        products[0].append(vu * zw - wz * yx)
        products[1].append(wz * xy - uv * zw)
        products[2].append(uv * yx)

    def spectral(comp):
        table = y_diff if comp == 2 else y_low
        return last([y_forward(value, cos, sin, table) for value in products[comp]])

    def to_inside(source, target, sems, count):
        for other in (others[i] for i in FAR):
            @pl.when(other <= LAST_RANK)
            def _(other=other):
                send(source, target, sems, count, count, other).start()

    modes_w = spectral(2)
    for e in range(2):
        send_w[pl.ds(e, 64, stride=2), :] = modes_w[:, 128 * e : 128 * e + 128]
    to_inside(send_w, recv_w, hz_sems, 2)
    for comp in range(2):
        modes_c = spectral(comp)
        for e in range(2):
            send_c[pl.ds(2 * comp + e, 64, stride=4), :] = modes_c[:, 128 * e : 128 * e + 128]
    to_inside(send_c, recv_c, c_sems, 4)

    inside = me <= LAST_RANK

    from_beside(halo)

    for comp in range(3):
        for i in range(2):
            for a in range(8):
                at = pl.ds(128 * a, 128)
                mid = vel[comp, 0, i, :, at]
                viscous = (high[comp, i, :, at] - 2.0 * mid + low[comp, i, :, at]) - (kx(a) * kx(a) + ky * ky) * mid
                out[comp, 0, i, :, at] = mid + (TIME_STEP * VISCOSITY) * viscous

    plain_cos = [jnp.broadcast_to(x_turn[0, c], (8, 128)) for c in range(8)]
    plain_sin = [jnp.broadcast_to(x_turn[1, c], (8, 128)) for c in range(8)]

    def add_nonlinear(comp, ref, base, stride):
        block = jnp.concatenate([ref[pl.ds(base + e, 64, stride=stride), :] for e in range(2)], 0)
        for a, pair in enumerate(x_forward(block, plain_cos, plain_sin, x_out)):
            at = pl.ds(128 * a, 128)
            keep = mask[:, at].astype(F32) * TIME_STEP
            for i in range(2):
                out[comp, 0, i, :, at] = out[comp, 0, i, :, at] + pair[i] * keep

    @pl.when(inside)
    def _():
        recv_w[rows(me, 2, 2), :] = send_w[rows(me, 2, 2), :]
        recv_c[rows(me, 4, 4), :] = send_c[rows(me, 4, 4), :]
        wait_all(recv_w, hz_sems.at[1], 2 * (RANKS - 1))
        add_nonlinear(2, recv_w, 0, 2)

    w_send[...] = out[2, 0]
    start_beside(w_halo)

    @pl.when(inside)
    def _():
        wait_all(recv_c, c_sems.at[1], 4 * (RANKS - 1))
        add_nonlinear(0, recv_c, 0, 4)
        add_nonlinear(1, recv_c, 2, 4)

    for a in range(8):
        at = pl.ds(128 * a, 128)
        div[0, 0, :, at] = -(kx(a) * out[0, 0, 1, :, at]) - ky * out[1, 0, 1, :, at]
        div[0, 1, :, at] = kx(a) * out[0, 0, 0, :, at] + ky * out[1, 0, 0, :, at]

    from_beside(w_halo)
    div[0] = div[0] + 0.5 * (w_high[...] - w_low[...])

    wait_all(send_u, u_sems.at[0], 4 * (RANKS - 1))
    wait_all(send_a, a_sems.at[0], 6 * (RANKS - 1))

    @pl.when(inside)
    def _():
        wait_all(send_w, hz_sems.at[0], 2 * LAST_RANK)
        wait_all(send_c, c_sems.at[0], 4 * LAST_RANK)

    @pl.when(jnp.logical_not(inside))
    def _():
        wait_all(send_w, hz_sems.at[0], 2 * (LAST_RANK + 1))
        wait_all(send_c, c_sems.at[0], 4 * (LAST_RANK + 1))

    for pair in (halo, *uv_halo, w_halo):
        left_beside(pair)


def store(following, divergence, out, div, sems):
    copies = [
        pltpu.make_async_copy(following, out, sems.at[0]),
        pltpu.make_async_copy(divergence, div, sems.at[1]),
    ]
    for copy in copies:
        copy.start()
    for copy in copies:
        copy.wait()


def on_device(velocity, mode_mask):
    constants = tables()
    operands = (velocity, mode_mask, *(jnp.asarray(constants[name]) for name in NAMES))
    whole = pl.BlockSpec(memory_space=pltpu.VMEM)
    dma, vmem = pltpu.SemaphoreType.DMA, pltpu.VMEM
    held = pl.pallas_call(
        kernel,
        name="substep",
        out_shape=(
            vmem((3, 1, 2, 8, 1024), F32),
            vmem((1, 2, 8, 1024), F32),
        ),
        in_specs=[pl.BlockSpec(memory_space=pl.ANY)] * len(operands),
        out_specs=(whole, whole),
        scratch_shapes=[
            *(vmem(operand.shape, operand.dtype) for operand in operands), dma((len(operands),)),
            vmem((256, 128), F32), vmem((256, 128), F32),
            vmem((512, 128), F32), vmem((512, 128), F32),
            vmem((128, 128), F32), vmem((128, 128), F32),
            vmem((256, 128), F32), vmem((256, 128), F32),
            *[vmem((2, 128, 128), F32)] * 3,
            *[vmem((3, 2, 8, 1024), F32)] * 2,
            *[vmem((2, 8, 1024), F32)] * 3,
            *[dma((2,))] * 4, dma((2, 4)), *[dma((4,))] * 2,
        ],
        compiler_params=pltpu.CompilerParams(collective_id=0, has_side_effects=True),
    )(*operands)
    return pl.pallas_call(
        store,
        name="store",
        out_shape=(
            jax.ShapeDtypeStruct((3, 1, 2, 8, 1024), F32),
            jax.ShapeDtypeStruct((1, 2, 8, 1024), F32),
        ),
        in_specs=[whole, whole],
        out_specs=[pl.BlockSpec(memory_space=pl.ANY)] * 2,
        scratch_shapes=[dma((2,))],
    )(*(pltpu.with_memory_space_constraint(value, pltpu.VMEM) for value in held))


def solution(mesh):
    return jax.shard_map(
        on_device,
        mesh=mesh,
        in_specs=(P(None, "gz", None, "pa", None), P("pa", None)),
        out_specs=(P(None, "gz", None, "pa", None), P("gz", None, "pa", None)),
        check_vma=False,
    )
```

```python
import math

import jax
import jax.numpy as jnp
import numpy as np
from jax import lax
from jax.experimental import pallas as pl
from jax.experimental.pallas import tpu as pltpu
from jax.sharding import PartitionSpec as P


TWO_PI = 2.0 * math.pi
TIME_STEP = 0.2
VISCOSITY = 0.25
RANKS = 64
LAST_RANK = 42
F32 = jnp.float32
BF16 = jnp.bfloat16


def halves(table):
    table = np.asarray(table, np.float32)
    high = table.astype(jnp.bfloat16)
    low = (table - high.astype(np.float32)).astype(jnp.bfloat16)
    return np.stack([high, low])


def tables():
    index = np.arange
    p, b, c, s, q, r = index(64), index(128), index(8), index(8), index(64), index(128)
    d = (2 * p[None, :] + index(2)[:, None]).reshape(-1)
    angle = TWO_PI / 128.0 * (d[:, None] * b[None, :] % 128)
    cos, sin = np.cos(angle) / 32.0, np.sin(angle) / 32.0
    x_in = np.block([[cos, -sin], [sin, cos]])
    angle = TWO_PI / 1024.0 * (c[:, None] * b[None, :])
    x_turn = np.stack([np.cos(angle), np.sin(angle)]).astype(np.float32).reshape(2, 8, 1, 128)
    angle = TWO_PI / 128.0 * (r[:, None] * q[None, :] % 128)
    cos, sin = np.cos(angle) / 32.0, np.sin(angle) / 32.0
    y_in = np.block([[cos, -sin], [sin, cos]])
    angle = TWO_PI / 1024.0 * (r[:, None] * np.tile(s, 16)[None, :])
    y_turn = np.stack([np.cos(angle), np.sin(angle)]).astype(np.float32)
    angle = TWO_PI / 8.0 * (s[:, None] * s[None, :] % 8)
    cos8, sin8 = np.cos(angle), np.sin(angle)
    eye = np.eye(8)
    real = np.kron(np.eye(2), np.kron(eye, cos8))
    imag = np.kron(np.eye(2), np.kron(eye, -sin8))
    both = np.concatenate([real, imag], 0)
    y_grid = np.concatenate([both, np.roll(both, 64, axis=1)], 1)
    real = np.kron(eye, cos8) / 32.0
    imag = np.kron(eye, -sin8) / 32.0
    line = np.concatenate([real, imag, imag, -real], 1)
    y_low = np.concatenate([line, np.zeros_like(line)], 0)
    y_diff = np.concatenate([line, -line], 0)
    angle = TWO_PI / 128.0 * (q[:, None] * r[None, :] % 128)
    y_out = np.concatenate([np.cos(angle), np.sin(angle)], 1)
    angle = TWO_PI / 128.0 * (d[:, None] * b[None, :] % 128)
    x_out = np.concatenate([np.cos(angle), np.sin(angle)], 1) / 32.0
    return dict(
        x_in=halves(x_in),
        x_turn=x_turn,
        y_in=halves(y_in),
        y_turn=y_turn,
        late=halves(np.concatenate([y_grid, y_low, y_diff, y_out, x_out], 0)),
    )


NAMES = ("x_in", "x_turn", "y_in", "y_turn", "late")
LATE = ((0, 256), (256, 128), (384, 128), (512, 64), (576, 128))


def split(value):
    high = value.astype(BF16)
    return high, (value - high.astype(F32)).astype(BF16)


def dot(left, right, contract=((1,), (0,))):
    def one(i, j):
        return lax.dot_general(left[i], right[j], (contract, ((), ())), preferred_element_type=F32)

    return one(0, 0) + (one(0, 1) + one(1, 0))


def eight(values, sign):
    count = len(values)
    if count == 1:
        return values
    even, odd = eight(values[0::2], sign), eight(values[1::2], sign)
    half = count // 2
    low, high = [], []
    for k in range(half):
        (er, ei), (qr, qi) = even[k], odd[k]
        turn = 8 // count * k
        if turn == 0:
            tr, ti = qr, qi
        elif turn == 2:
            tr, ti = -sign * qi, sign * qr
        else:
            root = math.sqrt(0.5)
            if turn == 1:
                tr, ti = root * (qr - sign * qi), root * (qi + sign * qr)
            else:
                tr, ti = -root * (qr + sign * qi), root * (sign * qr - qi)
        low.append((er + tr, ei + ti))
        high.append((er - tr, ei - ti))
    return low + high


def x_inverse(fields, turn_cos, turn_sin, table):
    real, imag = [], []
    for field in fields:
        for c, (vr, vi) in enumerate(eight(field, 1.0)):
            real.append(vr * turn_cos[c] - vi * turn_sin[c])
            imag.append(vr * turn_sin[c] + vi * turn_cos[c])
    lines = jnp.concatenate([jnp.concatenate(real, 0), jnp.concatenate(imag, 0)], 1)
    return dot(table, split(lines), ((1,), (1,)))


def y_turned(modes, cos, sin, table):
    lines = dot(table, split(modes))
    out = []
    for k in range(modes.shape[1] // 128):
        vr, vi = lines[:128, 128 * k : 128 * k + 128], lines[128:, 128 * k : 128 * k + 128]
        out.append(jnp.concatenate([vr * cos - vi * sin, vr * sin + vi * cos], 1))
    return out


def y_forward(product, cos, sin, table):
    line = dot(split(product), table)
    one, two = line[:, :128], line[:, 128:]
    return jnp.concatenate([one * cos + two * sin, two * cos - one * sin], 0)


def x_forward(block, turn_cos, turn_sin, table):
    line = dot(split(block.T), table)
    values = []
    for c in range(8):
        re, im = line[8 * c : 8 * c + 8], line[64 + 8 * c : 72 + 8 * c]
        vr, vi = re[:, :128] + im[:, 128:], im[:, :128] - re[:, 128:]
        values.append((vr * turn_cos[c] + vi * turn_sin[c], vi * turn_cos[c] - vr * turn_sin[c]))
    return eight(values, -1.0)


HOPS = [(dy, dz, dx) for dz in (1, 0) for dy in (4, 5, 3, 6, 2, 7, 1, 0) for dx in (2, 3, 1, 0)][:-1]
HOPS.sort(key=lambda hop: (-hop[1], -min(hop[0], 8 - hop[0]) - min(hop[2], 4 - hop[2])))


def hops(hop):
    dy, dz, dx = hop
    return min(dy, 8 - dy) + 4 * dz + min(dx, 4 - dx)


FAR = sorted(range(63), key=lambda i: -hops(HOPS[i]))


def partners(me):
    x, z, y = lax.rem(me, 4), lax.rem(lax.div(me, 4), 2), lax.div(me, 8)
    xs = [lax.rem(x + i, 4) for i in range(4)]
    zs = [4 * lax.rem(z + i, 2) for i in range(2)]
    ys = [8 * lax.rem(y + i, 8) for i in range(8)]
    return [ys[dy] + zs[dz] + xs[dx] for dy, dz, dx in HOPS]


def rows(start, align, count):
    return pl.ds(pl.multiple_of(start * align, align), count)


def kernel(*refs):
    count = 2 + len(NAMES)
    sources, out, div, held = refs[:count], refs[count], refs[count + 1], refs[count + 2 : 2 * count + 2]
    body(sources, held, out, div, *refs[2 * count + 2 :])


def body(sources, held, out, div, load_sems,
           send_u, recv_u, send_a, recv_a, send_w, recv_w, send_c, recv_c, uv_send, uv_low, uv_high,
           low, high, w_low, w_high, u_sems, a_sems, hz_sems, c_sems, uv_sems, halo_sems, w_sems):
    me, plane = lax.axis_index("pa"), lax.axis_index("gz")
    barrier = pltpu.get_barrier_semaphore()
    vel, mask, x_in, x_turn, y_in, y_turn, late_tables = held
    y_grid, y_low, y_diff, y_out, x_out = (late_tables.at[:, pl.ds(at, size)] for at, size in LATE)

    def load(i):
        return pltpu.make_async_copy(sources[i], held[i], load_sems.at[i])

    others = partners(me)
    for other in (others[i] for i in FAR):
        pl.semaphore_signal(barrier, inc=1, device_id={"gz": plane, "pa": other})
    has_low, has_high = plane > 0, plane < 7

    @pl.when(has_low)
    def _():
        pl.semaphore_signal(barrier, inc=1, device_id={"gz": plane - 1, "pa": me})

    @pl.when(has_high)
    def _():
        pl.semaphore_signal(barrier, inc=1, device_id={"gz": plane + 1, "pa": me})

    rest = [i for i in range(len(held)) if i not in (0, 2, 3)]
    for i in (0, 2, 3, *rest):
        load(i).start()
    sub = lax.broadcasted_iota(jnp.int32, (8, 128), 0)
    lane = lax.broadcasted_iota(jnp.int32, (8, 128), 1)
    modes = me * 8 + sub
    ky = (TWO_PI / 1024.0) * modes.astype(F32)
    weight = jnp.where(modes == 0, 1.0, 2.0).astype(F32)

    def kx(a):
        return (TWO_PI / 1024.0) * (lane + (128 * a - 1024 * (a // 4))).astype(F32)

    def piece(ref, *lead):
        return [ref[(*lead, slice(None), pl.ds(128 * a, 128))] for a in range(8)]

    for i in (0, 2, 3):
        load(i).wait()
    turn_cos = [weight * x_turn[0, c] for c in range(8)]
    turn_sin = [weight * x_turn[1, c] for c in range(8)]

    def field(comp):
        return list(zip(piece(vel, comp, 0, 0), piece(vel, comp, 0, 1), strict=True))

    u, v, w = field(0), field(1), field(2)
    omega_z = [
        (ky * u[a][1] - kx(a) * v[a][1], kx(a) * v[a][0] - ky * u[a][0]) for a in range(8)
    ]
    curl_y = [(kx(a) * w[a][1], -(kx(a) * w[a][0])) for a in range(8)]
    grid = x_inverse([u, v, w, omega_z, curl_y, curl_y], turn_cos, turn_sin, x_in)
    left = lax.broadcasted_iota(jnp.int32, (64, 128), 1) < 64
    for j in range(4):
        send_u[pl.ds(j, 64, stride=4), :] = grid[64 * j : 64 * j + 64, :128]
        send_a[pl.ds(j, 64, stride=8), :] = grid[64 * j : 64 * j + 64, 128:256]
    for ri in range(2):
        first, second = (grid[128 * ri + 64 * e : 128 * ri + 64 * e + 64, 256:] for e in range(2))
        send_a[pl.ds(4 + ri, 64, stride=8), :] = jnp.where(left, second, first)

    @pl.when(jnp.logical_and(has_low, has_high))
    def _():
        pl.semaphore_wait(barrier, RANKS + 1)

    @pl.when(jnp.logical_not(jnp.logical_and(has_low, has_high)))
    def _():
        pl.semaphore_wait(barrier, RANKS)

    def send(source, target, sems, align, count, dest):
        return pltpu.make_async_remote_copy(
            source.at[rows(dest, align, count)], target.at[rows(me, align, count)],
            sems.at[0], sems.at[1], device_id={"gz": plane, "pa": dest})

    for other in others:
        send(send_u, recv_u, u_sems, 4, 4, other).start()
    for other in others:
        send(send_a, recv_a, a_sems, 8, 6, other).start()

    def beside(source, target_low, target_high, sems):
        down = pltpu.make_async_remote_copy(
            source, target_high, sems.at[0], sems.at[1], device_id={"gz": plane - 1, "pa": me})
        up = pltpu.make_async_remote_copy(
            source, target_low, sems.at[2], sems.at[3], device_id={"gz": plane + 1, "pa": me})
        return down, up

    def start_beside(pair):
        @pl.when(has_low)
        def _():
            pair[0].start()

        @pl.when(has_high)
        def _():
            pair[1].start()

    def from_beside(pair):
        @pl.when(has_low)
        def _():
            pair[1].wait_recv()

        @pl.when(has_high)
        def _():
            pair[0].wait_recv()

    def left_beside(pair):
        @pl.when(has_low)
        def _():
            pair[0].wait_send()

        @pl.when(has_high)
        def _():
            pair[1].wait_send()

    halo = beside(vel.at[:, 0], low, high, halo_sems)
    uv_halo = [beside(uv_send.at[e], uv_low.at[e], uv_high.at[e], uv_sems.at[e]) for e in range(2)]
    w_halo = beside(out.at[2, 0], w_low, w_high, w_sems)

    @pl.when(jnp.logical_not(has_low))
    def _():
        low[...] = jnp.zeros_like(low)
        uv_low[...] = jnp.zeros_like(uv_low)
        w_low[...] = jnp.zeros_like(w_low)

    @pl.when(jnp.logical_not(has_high))
    def _():
        high[...] = jnp.zeros_like(high)
        uv_high[...] = jnp.zeros_like(uv_high)
        w_high[...] = jnp.zeros_like(w_high)

    recv_u[rows(me, 4, 4), :] = send_u[rows(me, 4, 4), :]
    recv_a[rows(me, 8, 6), :] = send_a[rows(me, 8, 6), :]

    def wait_all(ref, sem, count):
        view = ref.at[pl.ds(0, count)]
        pltpu.make_async_copy(view, view, sem).wait()

    for i in rest:
        load(i).wait()
    cos, sin = y_turn[0], y_turn[1]
    def gathered(ref, stride, e):
        return jnp.concatenate([ref[pl.ds(e, 64, stride=stride), :], ref[pl.ds(e + 2, 64, stride=stride), :]], 0)

    def on_grid(blocks):
        turned = y_turned(jnp.concatenate(blocks, 1), cos, sin, y_in)
        return [dot(split(value), y_grid) for value in turned]

    wait_all(recv_u, u_sems.at[1], 4 * (RANKS - 1))
    fields = []
    for e in range(2):
        fields += on_grid([gathered(recv_u, 4, e)])
        uv_send[e] = fields[e][:, :128]
        start_beside(uv_halo[e])
    wait_all(recv_a, a_sems.at[1], 6 * (RANKS - 1))
    start_beside(halo)
    row, col = (lax.broadcasted_iota(jnp.int32, (64, 128), i) for i in range(2))
    ky_grid = (TWO_PI / 1024.0) * (8 * row + lax.rem(col, 8)).astype(F32)
    blocks = [gathered(recv_a, 8, e) for e in range(2)]
    curl_re, curl_im = recv_a[pl.ds(4, 64, stride=8), :], recv_a[pl.ds(5, 64, stride=8), :]
    one, two = blocks[0], pltpu.roll(blocks[1], 64, 1)
    pair_one = [jnp.where(left, -(ky_grid * one[64:]), curl_re), jnp.where(left, ky_grid * one[:64], curl_im)]
    pair_two = [jnp.where(left, curl_re, -(ky_grid * two[64:])), jnp.where(left, curl_im, ky_grid * two[:64])]
    fields = fields + on_grid([*blocks, jnp.concatenate(pair_one, 0), jnp.concatenate(pair_two, 0)])
    for pair in uv_halo:
        from_beside(pair)

    def last(parts):
        return dot(y_out, split(jnp.concatenate(parts, 1)))

    sign = jnp.where(lax.broadcasted_iota(jnp.int32, (128, 128), 1) < 64, 0.5, -0.5).astype(F32)
    products = [[], [], []]
    for e in range(2):
        uv, wz, xy = fields[e], fields[2 + e], fields[4 + e]
        uv, vu = uv[:, :128], uv[:, 128:]
        wz, zw = wz[:, :128], wz[:, 128:]
        slope = sign * (uv_high[e] - uv_low[e])
        xy, yx = (xy[:, :128], xy[:, 128:]) if e == 0 else (xy[:, 128:], xy[:, :128])
        xy, yx = xy + pltpu.roll(slope, 64, 1), yx + slope
        products[0].append(vu * zw - wz * yx)
        products[1].append(wz * xy - uv * zw)
        products[2].append(uv * yx)

    def spectral(comp):
        table = y_diff if comp == 2 else y_low
        return last([y_forward(value, cos, sin, table) for value in products[comp]])

    def to_inside(source, target, sems, count):
        for other in (others[i] for i in FAR):
            @pl.when(other <= LAST_RANK)
            def _(other=other):
                send(source, target, sems, count, count, other).start()

    modes_w = spectral(2)
    for e in range(2):
        send_w[pl.ds(e, 64, stride=2), :] = modes_w[:, 128 * e : 128 * e + 128]
    to_inside(send_w, recv_w, hz_sems, 2)
    for comp in range(2):
        modes_c = spectral(comp)
        for e in range(2):
            send_c[pl.ds(2 * comp + e, 64, stride=4), :] = modes_c[:, 128 * e : 128 * e + 128]
    to_inside(send_c, recv_c, c_sems, 4)

    inside = me <= LAST_RANK

    from_beside(halo)

    for comp in range(3):
        for i in range(2):
            for a in range(8):
                at = pl.ds(128 * a, 128)
                mid = vel[comp, 0, i, :, at]
                viscous = (high[comp, i, :, at] - 2.0 * mid + low[comp, i, :, at]) - (kx(a) * kx(a) + ky * ky) * mid
                out[comp, 0, i, :, at] = mid + (TIME_STEP * VISCOSITY) * viscous

    plain_cos = [jnp.broadcast_to(x_turn[0, c], (8, 128)) for c in range(8)]
    plain_sin = [jnp.broadcast_to(x_turn[1, c], (8, 128)) for c in range(8)]

    def add_nonlinear(comp, ref, base, stride):
        block = jnp.concatenate([ref[pl.ds(base + e, 64, stride=stride), :] for e in range(2)], 0)
        for a, pair in enumerate(x_forward(block, plain_cos, plain_sin, x_out)):
            at = pl.ds(128 * a, 128)
            keep = mask[:, at].astype(F32) * TIME_STEP
            for i in range(2):
                out[comp, 0, i, :, at] = out[comp, 0, i, :, at] + pair[i] * keep

    @pl.when(inside)
    def _():
        recv_w[rows(me, 2, 2), :] = send_w[rows(me, 2, 2), :]
        recv_c[rows(me, 4, 4), :] = send_c[rows(me, 4, 4), :]
        wait_all(recv_w, hz_sems.at[1], 2 * (RANKS - 1))
        add_nonlinear(2, recv_w, 0, 2)

    start_beside(w_halo)

    @pl.when(inside)
    def _():
        wait_all(recv_c, c_sems.at[1], 4 * (RANKS - 1))
        add_nonlinear(0, recv_c, 0, 4)
        add_nonlinear(1, recv_c, 2, 4)

    for a in range(8):
        at = pl.ds(128 * a, 128)
        div[0, 0, :, at] = -(kx(a) * out[0, 0, 1, :, at]) - ky * out[1, 0, 1, :, at]
        div[0, 1, :, at] = kx(a) * out[0, 0, 0, :, at] + ky * out[1, 0, 0, :, at]

    from_beside(w_halo)
    div[0] = div[0] + 0.5 * (w_high[...] - w_low[...])

    wait_all(send_u, u_sems.at[0], 4 * (RANKS - 1))
    wait_all(send_a, a_sems.at[0], 6 * (RANKS - 1))

    @pl.when(inside)
    def _():
        wait_all(send_w, hz_sems.at[0], 2 * LAST_RANK)
        wait_all(send_c, c_sems.at[0], 4 * LAST_RANK)

    @pl.when(jnp.logical_not(inside))
    def _():
        wait_all(send_w, hz_sems.at[0], 2 * (LAST_RANK + 1))
        wait_all(send_c, c_sems.at[0], 4 * (LAST_RANK + 1))

    for pair in (halo, *uv_halo, w_halo):
        left_beside(pair)


def store(following, divergence, out, div, sems):
    copies = [
        pltpu.make_async_copy(following, out, sems.at[0]),
        pltpu.make_async_copy(divergence, div, sems.at[1]),
    ]
    for copy in copies:
        copy.start()
    for copy in copies:
        copy.wait()


def on_device(velocity, mode_mask):
    constants = tables()
    operands = (velocity, mode_mask, *(jnp.asarray(constants[name]) for name in NAMES))
    whole = pl.BlockSpec(memory_space=pltpu.VMEM)
    dma, vmem = pltpu.SemaphoreType.DMA, pltpu.VMEM
    held = pl.pallas_call(
        kernel,
        name="substep",
        out_shape=(
            vmem((3, 1, 2, 8, 1024), F32),
            vmem((1, 2, 8, 1024), F32),
        ),
        in_specs=[pl.BlockSpec(memory_space=pl.ANY)] * len(operands),
        out_specs=(whole, whole),
        scratch_shapes=[
            *(vmem(operand.shape, operand.dtype) for operand in operands), dma((len(operands),)),
            vmem((256, 128), F32), vmem((256, 128), F32),
            vmem((512, 128), F32), vmem((512, 128), F32),
            vmem((128, 128), F32), vmem((128, 128), F32),
            vmem((256, 128), F32), vmem((256, 128), F32),
            *[vmem((2, 128, 128), F32)] * 3,
            *[vmem((3, 2, 8, 1024), F32)] * 2,
            *[vmem((2, 8, 1024), F32)] * 2,
            *[dma((2,))] * 4, dma((2, 4)), *[dma((4,))] * 2,
        ],
        compiler_params=pltpu.CompilerParams(collective_id=0, has_side_effects=True),
    )(*operands)
    return pl.pallas_call(
        store,
        name="store",
        out_shape=(
            jax.ShapeDtypeStruct((3, 1, 2, 8, 1024), F32),
            jax.ShapeDtypeStruct((1, 2, 8, 1024), F32),
        ),
        in_specs=[whole, whole],
        out_specs=[pl.BlockSpec(memory_space=pl.ANY)] * 2,
        scratch_shapes=[dma((2,))],
    )(*(pltpu.with_memory_space_constraint(value, pltpu.VMEM) for value in held))


def solution(mesh):
    return jax.shard_map(
        on_device,
        mesh=mesh,
        in_specs=(P(None, "gz", None, "pa", None), P("pa", None)),
        out_specs=(P(None, "gz", None, "pa", None), P("gz", None, "pa", None)),
        check_vma=False,
    )
```

```python
import math

import jax
import jax.numpy as jnp
import numpy as np
from jax import lax
from jax.experimental import pallas as pl
from jax.experimental.pallas import tpu as pltpu
from jax.sharding import PartitionSpec as P


TWO_PI = 2.0 * math.pi
TIME_STEP = 0.2
VISCOSITY = 0.25
RANKS = 64
LAST_RANK = 42
F32 = jnp.float32
BF16 = jnp.bfloat16


def halves(table):
    table = np.asarray(table, np.float32)
    high = table.astype(jnp.bfloat16)
    low = (table - high.astype(np.float32)).astype(jnp.bfloat16)
    return np.stack([high, low])


def tables():
    index = np.arange
    p, b, c, s, q, r = index(64), index(128), index(8), index(8), index(64), index(128)
    d = (2 * p[None, :] + index(2)[:, None]).reshape(-1)
    angle = TWO_PI / 128.0 * (d[:, None] * b[None, :] % 128)
    cos, sin = np.cos(angle) / 32.0, np.sin(angle) / 32.0
    x_in = np.block([[cos, -sin], [sin, cos]])
    angle = TWO_PI / 1024.0 * (c[:, None] * b[None, :])
    x_turn = np.stack([np.cos(angle), np.sin(angle)]).astype(np.float32).reshape(2, 8, 1, 128)
    angle = TWO_PI / 128.0 * (r[:, None] * q[None, :] % 128)
    cos, sin = np.cos(angle) / 32.0, np.sin(angle) / 32.0
    y_in = np.block([[cos, -sin], [sin, cos]])
    angle = TWO_PI / 1024.0 * (r[:, None] * np.tile(s, 16)[None, :])
    y_turn = np.stack([np.cos(angle), np.sin(angle)]).astype(np.float32)
    angle = TWO_PI / 8.0 * (s[:, None] * s[None, :] % 8)
    cos8, sin8 = np.cos(angle), np.sin(angle)
    eye = np.eye(8)
    real = np.kron(np.eye(2), np.kron(eye, cos8))
    imag = np.kron(np.eye(2), np.kron(eye, -sin8))
    both = np.concatenate([real, imag], 0)
    y_grid = np.concatenate([both, np.roll(both, 64, axis=1)], 1)
    real = np.kron(eye, cos8) / 32.0
    imag = np.kron(eye, -sin8) / 32.0
    line = np.concatenate([real, imag, imag, -real], 1)
    y_low = np.concatenate([line, np.zeros_like(line)], 0)
    y_diff = np.concatenate([line, -line], 0)
    angle = TWO_PI / 128.0 * (q[:, None] * r[None, :] % 128)
    y_out = np.concatenate([np.cos(angle), np.sin(angle)], 1)
    angle = TWO_PI / 128.0 * (d[:, None] * b[None, :] % 128)
    x_out = np.concatenate([np.cos(angle), np.sin(angle)], 1) / 32.0
    return dict(
        x_in=halves(x_in),
        x_turn=x_turn,
        y_in=halves(y_in),
        y_turn=y_turn,
        late=halves(np.concatenate([y_grid, y_low, y_diff, y_out, x_out], 0)),
    )


NAMES = ("x_in", "x_turn", "y_in", "y_turn", "late")
LATE = ((0, 256), (256, 128), (384, 128), (512, 64), (576, 128))


def split(value):
    high = value.astype(BF16)
    return high, (value - high.astype(F32)).astype(BF16)


def dot(left, right, contract=((1,), (0,))):
    def one(i, j):
        return lax.dot_general(left[i], right[j], (contract, ((), ())), preferred_element_type=F32)

    return one(0, 0) + (one(0, 1) + one(1, 0))


def eight(values, sign):
    count = len(values)
    if count == 1:
        return values
    even, odd = eight(values[0::2], sign), eight(values[1::2], sign)
    half = count // 2
    low, high = [], []
    for k in range(half):
        (er, ei), (qr, qi) = even[k], odd[k]
        turn = 8 // count * k
        if turn == 0:
            tr, ti = qr, qi
        elif turn == 2:
            tr, ti = -sign * qi, sign * qr
        else:
            root = math.sqrt(0.5)
            if turn == 1:
                tr, ti = root * (qr - sign * qi), root * (qi + sign * qr)
            else:
                tr, ti = -root * (qr + sign * qi), root * (sign * qr - qi)
        low.append((er + tr, ei + ti))
        high.append((er - tr, ei - ti))
    return low + high


def x_inverse(fields, turn_cos, turn_sin, table):
    real, imag = [], []
    for field in fields:
        for c, (vr, vi) in enumerate(eight(field, 1.0)):
            real.append(vr * turn_cos[c] - vi * turn_sin[c])
            imag.append(vr * turn_sin[c] + vi * turn_cos[c])
    lines = jnp.concatenate([jnp.concatenate(real, 0), jnp.concatenate(imag, 0)], 1)
    return dot(table, split(lines), ((1,), (1,)))


def y_turned(modes, cos, sin, table):
    lines = dot(table, split(modes))
    out = []
    for k in range(modes.shape[1] // 128):
        vr, vi = lines[:128, 128 * k : 128 * k + 128], lines[128:, 128 * k : 128 * k + 128]
        out.append(jnp.concatenate([vr * cos - vi * sin, vr * sin + vi * cos], 1))
    return out


def y_forward(product, cos, sin, table):
    line = dot(split(product), table)
    one, two = line[:, :128], line[:, 128:]
    return jnp.concatenate([one * cos + two * sin, two * cos - one * sin], 0)


def x_forward(block, turn_cos, turn_sin, table):
    line = dot(split(block.T), table)
    values = []
    for c in range(8):
        re, im = line[8 * c : 8 * c + 8], line[64 + 8 * c : 72 + 8 * c]
        vr, vi = re[:, :128] + im[:, 128:], im[:, :128] - re[:, 128:]
        values.append((vr * turn_cos[c] + vi * turn_sin[c], vi * turn_cos[c] - vr * turn_sin[c]))
    return eight(values, -1.0)


HOPS = [(dy, dz, dx) for dz in (1, 0) for dy in (4, 5, 3, 6, 2, 7, 1, 0) for dx in (2, 3, 1, 0)][:-1]
HOPS.sort(key=lambda hop: (-hop[1], -min(hop[0], 8 - hop[0]) - min(hop[2], 4 - hop[2])))


def hops(hop):
    dy, dz, dx = hop
    return min(dy, 8 - dy) + 4 * dz + min(dx, 4 - dx)


FAR = sorted(range(63), key=lambda i: -hops(HOPS[i]))


def partners(me):
    x, z, y = lax.rem(me, 4), lax.rem(lax.div(me, 4), 2), lax.div(me, 8)
    xs = [lax.rem(x + i, 4) for i in range(4)]
    zs = [4 * lax.rem(z + i, 2) for i in range(2)]
    ys = [8 * lax.rem(y + i, 8) for i in range(8)]
    return [ys[dy] + zs[dz] + xs[dx] for dy, dz, dx in HOPS]


def rows(start, align, count):
    return pl.ds(pl.multiple_of(start * align, align), count)


def kernel(*refs):
    count = 2 + len(NAMES)
    sources, out, div, held = refs[:count], refs[count], refs[count + 1], refs[count + 2 : 2 * count + 2]
    body(sources, held, out, div, *refs[2 * count + 2 :])


def body(sources, held, out, div, load_sems,
           send_u, recv_u, send_a, recv_a, send_w, recv_w, send_c, recv_c, uv_send, uv_low, uv_high,
           low, high, w_low, w_high, u_sems, a_sems, hz_sems, c_sems, uv_sems, halo_sems, w_sems):
    me, plane = lax.axis_index("pa"), lax.axis_index("gz")
    barrier = pltpu.get_barrier_semaphore()
    vel, mask, x_in, x_turn, y_in, y_turn, late_tables = held
    y_grid, y_low, y_diff, y_out, x_out = (late_tables.at[:, pl.ds(at, size)] for at, size in LATE)

    def load(i):
        return pltpu.make_async_copy(sources[i], held[i], load_sems.at[i])

    others = partners(me)
    for other in (others[i] for i in FAR):
        pl.semaphore_signal(barrier, inc=1, device_id={"gz": plane, "pa": other})
    has_low, has_high = plane > 0, plane < 7

    @pl.when(has_low)
    def _():
        pl.semaphore_signal(barrier, inc=1, device_id={"gz": plane - 1, "pa": me})

    @pl.when(has_high)
    def _():
        pl.semaphore_signal(barrier, inc=1, device_id={"gz": plane + 1, "pa": me})

    rest = [i for i in range(len(held)) if i not in (0, 2, 3)]
    for i in (0, 2, 3, *rest):
        load(i).start()
    sub = lax.broadcasted_iota(jnp.int32, (8, 128), 0)
    lane = lax.broadcasted_iota(jnp.int32, (8, 128), 1)
    modes = me * 8 + sub
    ky = (TWO_PI / 1024.0) * modes.astype(F32)
    weight = jnp.where(modes == 0, 1.0, 2.0).astype(F32)

    def kx(a):
        return (TWO_PI / 1024.0) * (lane + (128 * a - 1024 * (a // 4))).astype(F32)

    def piece(ref, *lead):
        return [ref[(*lead, slice(None), pl.ds(128 * a, 128))] for a in range(8)]

    for i in (0, 2, 3):
        load(i).wait()
    turn_cos = [weight * x_turn[0, c] for c in range(8)]
    turn_sin = [weight * x_turn[1, c] for c in range(8)]

    def field(comp):
        return list(zip(piece(vel, comp, 0, 0), piece(vel, comp, 0, 1), strict=True))

    u, v, w = field(0), field(1), field(2)
    omega_z = [
        (ky * u[a][1] - kx(a) * v[a][1], kx(a) * v[a][0] - ky * u[a][0]) for a in range(8)
    ]
    curl_y = [(kx(a) * w[a][1], -(kx(a) * w[a][0])) for a in range(8)]
    grid = x_inverse([u, v, w, omega_z, curl_y, curl_y], turn_cos, turn_sin, x_in)
    left = lax.broadcasted_iota(jnp.int32, (64, 128), 1) < 64
    for j in range(4):
        send_u[pl.ds(j, 64, stride=4), :] = grid[64 * j : 64 * j + 64, :128]
        send_a[pl.ds(j, 64, stride=8), :] = grid[64 * j : 64 * j + 64, 128:256]
    for ri in range(2):
        first, second = (grid[128 * ri + 64 * e : 128 * ri + 64 * e + 64, 256:] for e in range(2))
        send_a[pl.ds(4 + ri, 64, stride=8), :] = jnp.where(left, second, first)

    @pl.when(jnp.logical_and(has_low, has_high))
    def _():
        pl.semaphore_wait(barrier, RANKS + 1)

    @pl.when(jnp.logical_not(jnp.logical_and(has_low, has_high)))
    def _():
        pl.semaphore_wait(barrier, RANKS)

    def send(source, target, sems, align, count, dest):
        return pltpu.make_async_remote_copy(
            source.at[rows(dest, align, count)], target.at[rows(me, align, count)],
            sems.at[0], sems.at[1], device_id={"gz": plane, "pa": dest})

    for other in others:
        send(send_u, recv_u, u_sems, 4, 4, other).start()
    for other in others:
        send(send_a, recv_a, a_sems, 8, 6, other).start()

    def beside(source, target_low, target_high, sems):
        down = pltpu.make_async_remote_copy(
            source, target_high, sems.at[0], sems.at[1], device_id={"gz": plane - 1, "pa": me})
        up = pltpu.make_async_remote_copy(
            source, target_low, sems.at[2], sems.at[3], device_id={"gz": plane + 1, "pa": me})
        return down, up

    def start_beside(pair):
        @pl.when(has_low)
        def _():
            pair[0].start()

        @pl.when(has_high)
        def _():
            pair[1].start()

    def from_beside(pair):
        @pl.when(has_low)
        def _():
            pair[1].wait_recv()

        @pl.when(has_high)
        def _():
            pair[0].wait_recv()

    def left_beside(pair):
        @pl.when(has_low)
        def _():
            pair[0].wait_send()

        @pl.when(has_high)
        def _():
            pair[1].wait_send()

    halo = beside(vel.at[:, 0], low, high, halo_sems)
    uv_halo = [beside(uv_send.at[e], uv_low.at[e], uv_high.at[e], uv_sems.at[e]) for e in range(2)]
    w_halo = beside(out.at[2, 0], w_low, w_high, w_sems)

    @pl.when(jnp.logical_not(has_low))
    def _():
        low[...] = jnp.zeros_like(low)
        uv_low[...] = jnp.zeros_like(uv_low)
        w_low[...] = jnp.zeros_like(w_low)

    @pl.when(jnp.logical_not(has_high))
    def _():
        high[...] = jnp.zeros_like(high)
        uv_high[...] = jnp.zeros_like(uv_high)
        w_high[...] = jnp.zeros_like(w_high)

    recv_u[rows(me, 4, 4), :] = send_u[rows(me, 4, 4), :]
    recv_a[rows(me, 8, 6), :] = send_a[rows(me, 8, 6), :]

    def wait_all(ref, sem, count):
        view = ref.at[pl.ds(0, count)]
        pltpu.make_async_copy(view, view, sem).wait()

    for i in rest:
        load(i).wait()
    cos, sin = y_turn[0], y_turn[1]
    def gathered(ref, stride, e):
        return jnp.concatenate([ref[pl.ds(e, 64, stride=stride), :], ref[pl.ds(e + 2, 64, stride=stride), :]], 0)

    def on_grid(blocks):
        turned = y_turned(jnp.concatenate(blocks, 1), cos, sin, y_in)
        return [dot(split(value), y_grid) for value in turned]

    wait_all(recv_u, u_sems.at[1], 4 * (RANKS - 1))
    fields = []
    for e in range(2):
        fields += on_grid([gathered(recv_u, 4, e)])
        uv_send[e] = fields[e][:, :128]
        start_beside(uv_halo[e])
    start_beside(halo)
    wait_all(recv_a, a_sems.at[1], 6 * (RANKS - 1))
    row, col = (lax.broadcasted_iota(jnp.int32, (64, 128), i) for i in range(2))
    ky_grid = (TWO_PI / 1024.0) * (8 * row + lax.rem(col, 8)).astype(F32)
    blocks = [gathered(recv_a, 8, e) for e in range(2)]
    curl_re, curl_im = recv_a[pl.ds(4, 64, stride=8), :], recv_a[pl.ds(5, 64, stride=8), :]
    one, two = blocks[0], pltpu.roll(blocks[1], 64, 1)
    pair_one = [jnp.where(left, -(ky_grid * one[64:]), curl_re), jnp.where(left, ky_grid * one[:64], curl_im)]
    pair_two = [jnp.where(left, curl_re, -(ky_grid * two[64:])), jnp.where(left, curl_im, ky_grid * two[:64])]
    fields = fields + on_grid([*blocks, jnp.concatenate(pair_one, 0), jnp.concatenate(pair_two, 0)])
    for pair in uv_halo:
        from_beside(pair)

    def last(parts):
        return dot(y_out, split(jnp.concatenate(parts, 1)))

    sign = jnp.where(lax.broadcasted_iota(jnp.int32, (128, 128), 1) < 64, 0.5, -0.5).astype(F32)
    products = [[], [], []]
    for e in range(2):
        uv, wz, xy = fields[e], fields[2 + e], fields[4 + e]
        uv, vu = uv[:, :128], uv[:, 128:]
        wz, zw = wz[:, :128], wz[:, 128:]
        slope = sign * (uv_high[e] - uv_low[e])
        xy, yx = (xy[:, :128], xy[:, 128:]) if e == 0 else (xy[:, 128:], xy[:, :128])
        xy, yx = xy + pltpu.roll(slope, 64, 1), yx + slope
        products[0].append(vu * zw - wz * yx)
        products[1].append(wz * xy - uv * zw)
        products[2].append(uv * yx)

    def spectral(comp):
        table = y_diff if comp == 2 else y_low
        return last([y_forward(value, cos, sin, table) for value in products[comp]])

    def to_inside(source, target, sems, count):
        for other in (others[i] for i in FAR):
            @pl.when(other <= LAST_RANK)
            def _(other=other):
                send(source, target, sems, count, count, other).start()

    modes_w = spectral(2)
    for e in range(2):
        send_w[pl.ds(e, 64, stride=2), :] = modes_w[:, 128 * e : 128 * e + 128]
    to_inside(send_w, recv_w, hz_sems, 2)
    for comp in range(2):
        modes_c = spectral(comp)
        for e in range(2):
            send_c[pl.ds(2 * comp + e, 64, stride=4), :] = modes_c[:, 128 * e : 128 * e + 128]
    to_inside(send_c, recv_c, c_sems, 4)

    inside = me <= LAST_RANK

    from_beside(halo)

    for comp in range(3):
        for i in range(2):
            for a in range(8):
                at = pl.ds(128 * a, 128)
                mid = vel[comp, 0, i, :, at]
                viscous = (high[comp, i, :, at] - 2.0 * mid + low[comp, i, :, at]) - (kx(a) * kx(a) + ky * ky) * mid
                out[comp, 0, i, :, at] = mid + (TIME_STEP * VISCOSITY) * viscous

    plain_cos = [jnp.broadcast_to(x_turn[0, c], (8, 128)) for c in range(8)]
    plain_sin = [jnp.broadcast_to(x_turn[1, c], (8, 128)) for c in range(8)]

    def add_nonlinear(comp, ref, base, stride):
        block = jnp.concatenate([ref[pl.ds(base + e, 64, stride=stride), :] for e in range(2)], 0)
        for a, pair in enumerate(x_forward(block, plain_cos, plain_sin, x_out)):
            at = pl.ds(128 * a, 128)
            keep = mask[:, at].astype(F32) * TIME_STEP
            for i in range(2):
                out[comp, 0, i, :, at] = out[comp, 0, i, :, at] + pair[i] * keep

    @pl.when(inside)
    def _():
        recv_w[rows(me, 2, 2), :] = send_w[rows(me, 2, 2), :]
        recv_c[rows(me, 4, 4), :] = send_c[rows(me, 4, 4), :]
        wait_all(recv_w, hz_sems.at[1], 2 * (RANKS - 1))
        add_nonlinear(2, recv_w, 0, 2)

    start_beside(w_halo)

    @pl.when(inside)
    def _():
        wait_all(recv_c, c_sems.at[1], 4 * (RANKS - 1))
        add_nonlinear(0, recv_c, 0, 4)
        add_nonlinear(1, recv_c, 2, 4)

    for a in range(8):
        at = pl.ds(128 * a, 128)
        div[0, 0, :, at] = -(kx(a) * out[0, 0, 1, :, at]) - ky * out[1, 0, 1, :, at]
        div[0, 1, :, at] = kx(a) * out[0, 0, 0, :, at] + ky * out[1, 0, 0, :, at]

    from_beside(w_halo)
    div[0] = div[0] + 0.5 * (w_high[...] - w_low[...])

    wait_all(send_u, u_sems.at[0], 4 * (RANKS - 1))
    wait_all(send_a, a_sems.at[0], 6 * (RANKS - 1))

    @pl.when(inside)
    def _():
        wait_all(send_w, hz_sems.at[0], 2 * LAST_RANK)
        wait_all(send_c, c_sems.at[0], 4 * LAST_RANK)

    @pl.when(jnp.logical_not(inside))
    def _():
        wait_all(send_w, hz_sems.at[0], 2 * (LAST_RANK + 1))
        wait_all(send_c, c_sems.at[0], 4 * (LAST_RANK + 1))

    for pair in (halo, *uv_halo, w_halo):
        left_beside(pair)


def store(following, divergence, out, div, sems):
    copies = [
        pltpu.make_async_copy(following, out, sems.at[0]),
        pltpu.make_async_copy(divergence, div, sems.at[1]),
    ]
    for copy in copies:
        copy.start()
    for copy in copies:
        copy.wait()


def on_device(velocity, mode_mask):
    constants = tables()
    operands = (velocity, mode_mask, *(jnp.asarray(constants[name]) for name in NAMES))
    whole = pl.BlockSpec(memory_space=pltpu.VMEM)
    dma, vmem = pltpu.SemaphoreType.DMA, pltpu.VMEM
    held = pl.pallas_call(
        kernel,
        name="substep",
        out_shape=(
            vmem((3, 1, 2, 8, 1024), F32),
            vmem((1, 2, 8, 1024), F32),
        ),
        in_specs=[pl.BlockSpec(memory_space=pl.ANY)] * len(operands),
        out_specs=(whole, whole),
        scratch_shapes=[
            *(vmem(operand.shape, operand.dtype) for operand in operands), dma((len(operands),)),
            vmem((256, 128), F32), vmem((256, 128), F32),
            vmem((512, 128), F32), vmem((512, 128), F32),
            vmem((128, 128), F32), vmem((128, 128), F32),
            vmem((256, 128), F32), vmem((256, 128), F32),
            *[vmem((2, 128, 128), F32)] * 3,
            *[vmem((3, 2, 8, 1024), F32)] * 2,
            *[vmem((2, 8, 1024), F32)] * 2,
            *[dma((2,))] * 4, dma((2, 4)), *[dma((4,))] * 2,
        ],
        compiler_params=pltpu.CompilerParams(collective_id=0, has_side_effects=True),
    )(*operands)
    return pl.pallas_call(
        store,
        name="store",
        out_shape=(
            jax.ShapeDtypeStruct((3, 1, 2, 8, 1024), F32),
            jax.ShapeDtypeStruct((1, 2, 8, 1024), F32),
        ),
        in_specs=[whole, whole],
        out_specs=[pl.BlockSpec(memory_space=pl.ANY)] * 2,
        scratch_shapes=[dma((2,))],
    )(*(pltpu.with_memory_space_constraint(value, pltpu.VMEM) for value in held))


def solution(mesh):
    return jax.shard_map(
        on_device,
        mesh=mesh,
        in_specs=(P(None, "gz", None, "pa", None), P("pa", None)),
        out_specs=(P(None, "gz", None, "pa", None), P("gz", None, "pa", None)),
        check_vma=False,
    )
```
